8 devices in a mesh: dp: 2 (over z, y), tp: 4 (over x, core).
Axes of the slice: x: 2, y: 2, z: 1, core: 2. Of those that a mesh axis runs over, the one named last changes fastest.
Arguments:
- x: bfloat16 [4096, 2048], P('dp'), parts along dimension 0
- mu1: float32 [4096], P('dp'), parts along dimension 0
- rs1: float32 [4096], P('dp'), parts along dimension 0
- g1: bfloat16 [2048], replicated
- g2: bfloat16 [2048], replicated
- dy: bfloat16 [4096, 2048], P('dp'), parts along dimension 0
- wqkv: bfloat16 [2048, 6144], P(None, 'tp')
- wo: bfloat16 [32, 64, 2048], P('tp')
- w1: bfloat16 [2048, 8192], P(None, 'tp')
- w2: bfloat16 [8192, 2048], P('tp')
Outputs:
- output 1: bfloat16 [4096, 2048], P('dp'), parts along dimension 0
- output 2: bfloat16 [4096, 6144], P('dp', 'tp'), parts along dimension 0
- output 3: bfloat16 [64, 64, 2048], P(('dp', 'tp')), parts along dimension 0
- output 4: bfloat16 [4096, 8192], P('dp', 'tp'), parts along dimension 0
- output 5: bfloat16 [16384, 2048], P(('dp', 'tp')), parts along dimension 0
There are 2 independent parts. The reference program is written for one: setup_inputs(seed, part) draws one part's arguments, and reference() takes and returns one part's arrays. A program takes and returns all parts, laid end to end along the dimension named above; an argument that names none is the same for every part.
All inputs are finite; a program needn't handle non-finite values.
Results may differ from the reference program's by a relative error of at most 0.0158731.
Values are sent between devices in bfloat16 or wider.
A program may use at most 1 GiB of HBM per device.

```python
import jax
import jax.numpy as jnp
from jax import lax

T = 2048
D = 2048
HEADS = 32
FF = 8192
HEAD = D // HEADS
EPS = 1.0 / 100000
QK_GAIN = 2.5 ** 0.5


def setup_inputs(seed: int = 0, part: int = 0) -> dict:
    kp = jax.random.fold_in(jax.random.key(seed), part)
    ka = jax.random.split(kp, 4)
    kw = jax.random.split(jax.random.key(seed + 1), 6)
    z = jax.random.normal(ka[0], (T, D), jnp.float32)
    z = z - jnp.mean(z, axis=-1, keepdims=True)
    z = z * lax.rsqrt(jnp.mean(z * z, axis=-1, keepdims=True))
    mu1 = 0.5 * jax.random.normal(ka[1], (T,), jnp.float32)
    rs1 = jax.random.uniform(ka[2], (T,), jnp.float32, 0.7, 1.4)
    x = (mu1[:, None] + z / rs1[:, None]).astype(jnp.bfloat16)
    dy = jax.random.normal(ka[3], (T, D), jnp.float32).astype(jnp.bfloat16)
    g1 = jax.random.uniform(kw[0], (D,), jnp.float32, 0.6, 1.4).astype(jnp.bfloat16)
    g2 = jax.random.uniform(kw[1], (D,), jnp.float32, 0.6, 1.4).astype(jnp.bfloat16)
    gain = jnp.array([QK_GAIN, QK_GAIN, 1.0], jnp.float32)[None, None, :, None]
    wqkv = jax.random.normal(kw[2], (D, HEADS, 3, HEAD), jnp.float32) * gain * D ** -0.5
    wo = jax.random.normal(kw[3], (HEADS, HEAD, D), jnp.float32) * D ** -0.5
    w1 = jax.random.normal(kw[4], (D, FF), jnp.float32) * D ** -0.5
    w2 = jax.random.normal(kw[5], (FF, D), jnp.float32) * FF ** -0.5
    return {"x": x, "mu1": mu1, "rs1": rs1, "g1": g1, "g2": g2, "dy": dy,
            "wqkv": wqkv.reshape(D, 3 * D).astype(jnp.bfloat16), "wo": wo.astype(jnp.bfloat16),
            "w1": w1.astype(jnp.bfloat16), "w2": w2.astype(jnp.bfloat16)}


def _ln_bwd(dn, xh, rs, g):
    u = dn * g
    return rs[:, None] * (u - jnp.mean(u, axis=-1, keepdims=True) - xh * jnp.mean(u * xh, axis=-1, keepdims=True))


def _probs(q, k):
    s = jnp.dot(q, k.T, preferred_element_type=jnp.float32) * HEAD ** -0.5
    mask = jnp.arange(T)[:, None] >= jnp.arange(T)[None, :]
    return jax.nn.softmax(jnp.where(mask, s, -jnp.inf), axis=-1)


def _head_fwd(qkv):
    q, k, v = qkv[:, 0], qkv[:, 1], qkv[:, 2]
    p = _probs(q, k)
    return jnp.dot(p.astype(jnp.bfloat16), v, preferred_element_type=jnp.float32).astype(jnp.bfloat16)


def _head_bwd(args):
    qkv, do = args
    q, k, v = qkv[:, 0], qkv[:, 1], qkv[:, 2]
    p = _probs(q, k)
    dv = jnp.dot(p.astype(jnp.bfloat16).T, do, preferred_element_type=jnp.float32)
    dpm = jnp.dot(do, v.T, preferred_element_type=jnp.float32)
    ds = (p * (dpm - jnp.sum(p * dpm, axis=-1, keepdims=True)) * HEAD ** -0.5).astype(jnp.bfloat16)
    dq = jnp.dot(ds, k, preferred_element_type=jnp.float32)
    dk = jnp.dot(ds.T, q, preferred_element_type=jnp.float32)
    return jnp.stack([dq, dk, dv], axis=1).astype(jnp.bfloat16)


def reference(x, mu1, rs1, g1, g2, dy, wqkv, wo, w1, w2):
    xf = x.astype(jnp.float32)
    g1f = g1.astype(jnp.float32)
    g2f = g2.astype(jnp.float32)
    xh1 = (xf - mu1[:, None]) * rs1[:, None]
    n1 = (xh1 * g1f).astype(jnp.bfloat16)
    qkv = jnp.dot(n1, wqkv, preferred_element_type=jnp.float32).astype(jnp.bfloat16)
    qkv = jnp.moveaxis(qkv.reshape(T, HEADS, 3, HEAD), 1, 0)
    o = lax.map(_head_fwd, qkv)
    o = jnp.moveaxis(o, 0, 1).reshape(T, D)
    wo2 = wo.reshape(D, D)
    h1 = xf + jnp.dot(o, wo2, preferred_element_type=jnp.float32)
    mu2 = jnp.mean(h1, axis=-1, keepdims=True)
    xc = h1 - mu2
    rs2 = lax.rsqrt(jnp.mean(xc * xc, axis=-1) + EPS)
    xh2 = xc * rs2[:, None]
    n2 = (xh2 * g2f).astype(jnp.bfloat16)
    a = jnp.dot(n2, w1, preferred_element_type=jnp.float32)
    gl, gelu_vjp = jax.vjp(jax.nn.gelu, a)
    gb = gl.astype(jnp.bfloat16)
    dw2 = jnp.dot(gb.T, dy, preferred_element_type=jnp.float32).astype(jnp.bfloat16)
    dg = jnp.dot(dy, w2.T, preferred_element_type=jnp.float32)
    da = gelu_vjp(dg)[0].astype(jnp.bfloat16)
    dw1 = jnp.dot(n2.T, da, preferred_element_type=jnp.float32).astype(jnp.bfloat16)
    dn2 = jnp.dot(da, w1.T, preferred_element_type=jnp.float32)
    dh1 = dy.astype(jnp.float32) + _ln_bwd(dn2, xh2, rs2, g2f)
    dh1b = dh1.astype(jnp.bfloat16)
    dwo = jnp.dot(o.T, dh1b, preferred_element_type=jnp.float32).astype(jnp.bfloat16).reshape(HEADS, HEAD, D)
    do = jnp.dot(dh1b, wo2.T, preferred_element_type=jnp.float32).astype(jnp.bfloat16)
    do = jnp.moveaxis(do.reshape(T, HEADS, HEAD), 1, 0)
    dqkv = lax.map(_head_bwd, (qkv, do))
    dqkv = jnp.moveaxis(dqkv, 0, 1).reshape(T, 3 * D)
    dwqkv = jnp.dot(n1.T, dqkv, preferred_element_type=jnp.float32).astype(jnp.bfloat16)
    dn1 = jnp.dot(dqkv, wqkv.T, preferred_element_type=jnp.float32)
    dx = (dh1 + _ln_bwd(dn1, xh1, rs1, g1f)).astype(jnp.bfloat16)
    return dx, dwqkv, dwo, dw1, dw2
```

```python
import functools

import jax
import jax.numpy as jnp
from jax import lax
from jax.experimental import pallas as pl
from jax.experimental.pallas import tpu as pltpu
from jax.sharding import PartitionSpec as P

EPS = 1.0 / 100000
LOG2E = 1.4426950408889634
f32 = jnp.float32
bf = jnp.bfloat16
NB = 4
BQ = 256
MB = 2**20
SAME = [(0, 1), (1, 0), (2, 3), (3, 2)]
CROSS = [(0, 2), (2, 0), (1, 3), (3, 1)]


def _dot(a, b):
    return jnp.dot(a, b, preferred_element_type=f32)


def _dot_t(a, b):
    return lax.dot_general(a, b, (((1,), (1,)), ((), ())), preferred_element_type=f32)


def _causal(n):
    return lax.broadcasted_iota(jnp.int32, (n, n), 0) >= lax.broadcasted_iota(jnp.int32, (n, n), 1)


def _params(mb=60):
    return pltpu.CompilerParams(vmem_limit_bytes=mb * MB)


def _cost(flops, nbytes):
    return pl.CostEstimate(flops=int(flops), bytes_accessed=int(nbytes), transcendentals=0)


def _fwd_kernel(qkv_ref, o_ref, lse_ref, k_t, v_t, q_s, *, t, hd):
    c = LOG2E * hd**-0.5
    for h in range(2):
        b = 3 * hd * h
        q_s[h] = qkv_ref[:, b : b + hd]
        k_t[h] = qkv_ref[:, b + hd : b + 2 * hd].T
        v_t[h] = qkv_ref[:, b + 2 * hd : b + 3 * hd].T
    for i in range(t // BQ):
        w = (i + 1) * BQ
        rows = slice(i * BQ, w)
        outs = []
        for h in range(2):
            s = _dot(q_s[h, rows, :], k_t[h, :, :w])
            d = jnp.where(_causal(BQ), s[:, w - BQ :], -jnp.inf)
            s = jnp.concatenate([s[:, : w - BQ], d], 1) if i else d
            m = jnp.max(s, axis=1, keepdims=True)
            p = jnp.exp2((s - m) * c)
            l = jnp.sum(p, axis=1, keepdims=True)
            outs.append(_dot_t(v_t[h, :, :w], p.astype(bf)).T * (1.0 / l))
            lse_ref[0, h : h + 1, rows] = (m * c + jnp.log2(l)).T
        o_ref[rows, :] = jnp.concatenate(outs, 1).astype(bf)


def _attn_fwd(qkv, hd, first, npair):
    t = qkv.shape[0]
    return pl.pallas_call(
        functools.partial(_fwd_kernel, t=t, hd=hd),
        grid=(npair,),
        in_specs=[pl.BlockSpec((t, 6 * hd), lambda p: (0, p + first))],
        out_specs=[pl.BlockSpec((t, 2 * hd), lambda p: (0, p)), pl.BlockSpec((1, 2, t), lambda p: (p, 0, 0))],
        out_shape=[jax.ShapeDtypeStruct((t, npair * 2 * hd), bf), jax.ShapeDtypeStruct((npair, 2, t), f32)],
        scratch_shapes=[pltpu.VMEM((2, hd, t), bf), pltpu.VMEM((2, hd, t), bf), pltpu.VMEM((2, t, hd), bf)],
        compiler_params=_params(),
        cost_estimate=_cost(npair * 9.5e9, npair * 2 * t * hd * 16),
        name="attn_fwd",
    )(qkv)


def _bwd_kernel(*refs, hd, r0, r1, has_in, has_out, half):
    qkv_ref, o0_ref, o1_ref, do_ref, lse0_ref, lse1_ref = refs[:6]
    refs = refs[6:]
    acc_in = None
    if has_in:
        acc_in, _ = refs[:2]
        refs = refs[2:]
    out_ref, full_ref = refs[:2]
    refs = refs[2:]
    acc_out = None
    if has_out:
        acc_out = refs[0]
        refs = refs[1:]
    q_t, k_t, v_t, do_t, q_s, do_s, dk_t, dv_t = refs
    sc = hd**-0.5
    c = LOG2E * sc
    first_half = pl.program_id(0) < half
    for h in range(2):
        b = 3 * hd * h
        q = qkv_ref[r0:r1, b : b + hd]
        do = do_ref[:, h * hd : (h + 1) * hd]
        q_s[h] = q
        do_s[h] = do
        q_t[h] = q.T
        do_t[h] = do.T
        k_t[h] = qkv_ref[:, b + hd : b + 2 * hd].T
        v_t[h] = qkv_ref[:, b + 2 * hd : b + 3 * hd].T
        if has_in:
            dk_t[h] = acc_in[0, 2 * hd * h : 2 * hd * h + hd, :]
            dv_t[h] = acc_in[0, 2 * hd * h + hd : 2 * hd * h + 2 * hd, :]
    for i in reversed(range(r0 // BQ, r1 // BQ)):
        w = (i + 1) * BQ
        rows = slice(i * BQ, w)
        loc = slice(i * BQ - r0, w - r0)
        outs = []
        for h in range(2):
            lse = jnp.where(first_half, lse0_ref[0, h : h + 1, rows], lse1_ref[0, h : h + 1, rows]).T
            hs = slice(h * hd, (h + 1) * hd)
            o = jnp.where(first_half, o0_ref[loc, hs], o1_ref[loc, hs])
            delta = jnp.sum(do_ref[loc, hs].astype(f32) * o.astype(f32), axis=1, keepdims=True)
            p = jnp.exp2(_dot(q_s[h, loc, :], k_t[h, :, :w]) * c - lse)
            d = jnp.where(_causal(BQ), p[:, w - BQ :], 0.0)
            p = jnp.concatenate([p[:, : w - BQ], d], 1) if i else d
            dp = _dot(do_s[h, loc, :], v_t[h, :, :w])
            ds = (p * (dp - delta)).astype(bf)
            dv = _dot(do_t[h, :, loc], p.astype(bf))
            dk = _dot(q_t[h, :, loc], ds)
            if w == r1 and not has_in:
                dv_t[h] = dv
                dk_t[h] = dk
            else:
                dv_t[h, :, :w] += dv
                dk_t[h, :, :w] += dk
            dq = _dot_t(k_t[h, :, :w], ds).T
            outs.append((dq * sc).astype(bf))
            outs.append((dk_t[h, :, rows] * sc).T.astype(bf))
            outs.append(dv_t[h, :, rows].T.astype(bf))
        res = jnp.concatenate(outs, 1)
        out_ref[loc, :] = res
        full_ref[loc, :] = res
    if has_out:
        for h in range(2):
            acc_out[0, 2 * hd * h : 2 * hd * h + hd, :] = dk_t[h, :, :r0]
            acc_out[0, 2 * hd * h + hd : 2 * hd * h + 2 * hd, :] = dv_t[h, :, :r0]


def _attn_bwd(qkv, o0, o1, do, lse0, lse1, acc, full, chunk, b, hd):
    t, w = qkv.shape
    npair = w // (6 * hd)
    half = npair // 2
    r0, r1 = chunk * b, (chunk + 1) * b
    has_in, has_out = acc is not None, r0 > 0
    lo = lambda p: jnp.minimum(p, half - 1)
    hi = lambda p: jnp.maximum(p - half, 0)
    in_specs = [
        pl.BlockSpec((r1, 6 * hd), lambda p: (0, p)),
        pl.BlockSpec((b, 2 * hd), lambda p: (chunk, lo(p))),
        pl.BlockSpec((b, 2 * hd), lambda p: (chunk, hi(p))),
        pl.BlockSpec((b, 2 * hd), lambda p: (0, p)),
        pl.BlockSpec((1, 2, t), lambda p: (lo(p), 0, 0)),
        pl.BlockSpec((1, 2, t), lambda p: (hi(p), 0, 0)),
    ]
    args = [qkv, o0, o1, do, lse0, lse1]
    alias = {}
    if has_in:
        in_specs += [pl.BlockSpec((1, 4 * hd, r1), lambda p: (p, 0, 0)), pl.BlockSpec(memory_space=pl.ANY)]
        args += [acc, full]
        alias = {7: 1}
    out_specs = [pl.BlockSpec((b, 6 * hd), lambda p: (0, p)), pl.BlockSpec((b, 6 * hd), lambda p: (chunk, p))]
    out_shape = [jax.ShapeDtypeStruct((b, w), bf), jax.ShapeDtypeStruct((t, w), bf)]
    if has_out:
        out_specs.append(pl.BlockSpec((1, 4 * hd, r0), lambda p: (p, 0, 0)))
        out_shape.append(jax.ShapeDtypeStruct((npair, 4 * hd, r0), f32))
    work = npair * 2 * b * (r0 + r1)
    return pl.pallas_call(
        functools.partial(_bwd_kernel, hd=hd, r0=r0, r1=r1, has_in=has_in, has_out=has_out, half=half),
        grid=(npair,),
        in_specs=in_specs,
        out_specs=out_specs,
        out_shape=out_shape,
        scratch_shapes=[
            pltpu.VMEM((2, hd, b), bf), pltpu.VMEM((2, hd, r1), bf), pltpu.VMEM((2, hd, r1), bf), pltpu.VMEM((2, hd, b), bf),
            pltpu.VMEM((2, b, hd), bf), pltpu.VMEM((2, b, hd), bf), pltpu.VMEM((2, hd, r1), f32), pltpu.VMEM((2, hd, r1), f32),
        ],
        input_output_aliases=alias,
        compiler_params=_params(),
        cost_estimate=_cost(work * 1500, 3 * t * w),
        name=f"attn_bwd_{chunk}",
    )(*args)


def _h1_kernel(ids, x_ref, oa, ob, pa, pb, qa, qb, ra, rb, wa, wb, wc, wd, g_ref, xh_ref, rs_ref, own_ref, full_ref, acc):
    def run(first, second):
        acc[...] = sum(_dot(jnp.concatenate([u, v], 1), w[...]) for u, v, w in first + second)

    near = [(oa[0, 0], ob[0, 0], wa), (pa[0], pb[0], wb)]
    far = [(qa[0, 0], qb[0, 0], wc), (ra[0], rb[0], wd)]

    @pl.when(ids[1] == 0)
    def _():
        run(near, far)

    @pl.when(ids[1] != 0)
    def _():
        run(far, near)

    h1 = x_ref[0, 0].astype(f32) + acc[...]
    xc = h1 - jnp.mean(h1, axis=1, keepdims=True)
    rs = lax.rsqrt(jnp.mean(xc * xc, axis=1, keepdims=True) + EPS)
    xh = xc * rs
    n2 = (xh * g_ref[...].astype(f32)).astype(bf)
    xh_ref[0] = xh
    rs_ref[0] = jnp.broadcast_to(rs, (rs.shape[0], 128))
    own_ref[0] = n2
    full_ref[0, 0] = n2


def _h1(ids, x4, o_own, o_same, o_cross, o_diag, ws, g2):
    nb, _, r, d = x4.shape
    own = lambda k: pl.BlockSpec((1, 1, r, k), lambda i, s: (i, s[0], 0, 0))
    row = lambda k: pl.BlockSpec((1, r, k), lambda i, s: (i, 0, 0))
    const = lambda shape: pl.BlockSpec(shape, lambda i, s: (0, 0), pipeline_mode=pl.Buffered(1))
    k = o_own[0].shape[-1]
    return pl.pallas_call(
        _h1_kernel,
        grid_spec=pltpu.PrefetchScalarGridSpec(
            num_scalar_prefetch=1,
            grid=(nb,),
            in_specs=[own(d), own(k), own(k), row(k), row(k), own(k), own(k), row(k), row(k)]
            + [const((2 * k, d))] * 4
            + [const((1, d))],
            out_specs=[row(d), row(128), row(d), own(d)],
            scratch_shapes=[pltpu.VMEM((r, d), f32)],
        ),
        out_shape=[
            jax.ShapeDtypeStruct((nb, r, d), f32),
            jax.ShapeDtypeStruct((nb, r, 128), f32),
            jax.ShapeDtypeStruct((nb, r, d), bf),
            jax.ShapeDtypeStruct((nb, 2, r, d), bf),
        ],
        compiler_params=_params(),
        cost_estimate=_cost(2 * nb * r * d * 8 * k, 30 * MB),
        name="h1_norm",
    )(ids, x4, *o_own, *o_same, *o_cross, *o_diag, *ws, g2)


def _lnb2_kernel(ids, sa, sb, xh_ref, rs_ref, dy_ref, g_ref, dh_ref, dhb_ref):
    u = (sa[...].astype(f32) + sb[...].astype(f32)) * g_ref[...].astype(f32)
    xh = xh_ref[0]
    v = u - jnp.mean(u, axis=1, keepdims=True) - xh * jnp.mean(u * xh, axis=1, keepdims=True)
    dh = dy_ref[0, 0].astype(f32) + rs_ref[0][:, :1] * v
    dh_ref[...] = dh
    dhb_ref[...] = dh.astype(bf)


def _lnb1_kernel(ids, sa, sb, x_ref, mu_ref, rs_ref, dh_ref, g_ref, dx_ref):
    u = (sa[...].astype(f32) + sb[...].astype(f32)) * g_ref[...].astype(f32)
    rs = rs_ref[0, 0].T
    xh = (x_ref[0, 0].astype(f32) - mu_ref[0, 0].T) * rs
    v = u - jnp.mean(u, axis=1, keepdims=True) - xh * jnp.mean(u * xh, axis=1, keepdims=True)
    dx_ref[...] = (dh_ref[...] + rs * v).astype(bf)


def _lnb(kernel, ids, sa, sb, mids, mid_specs, g, outs, name, chunk, tile=128):
    r, d = sa.shape
    tile = min(tile, r)
    flat = lambda k: pl.BlockSpec((tile, k), lambda i, s: (i, 0))
    specs = {
        "row": lambda k: pl.BlockSpec((1, tile, k), lambda i, s: (chunk, i, 0)),
        "own": lambda k: pl.BlockSpec((1, 1, tile, k), lambda i, s: (chunk, s[0], i, 0)),
        "stat": lambda k: pl.BlockSpec((1, 1, 1, tile), lambda i, s: (chunk, s[0], 0, i)),
        "flat": flat,
    }
    return pl.pallas_call(
        kernel,
        grid_spec=pltpu.PrefetchScalarGridSpec(
            num_scalar_prefetch=1,
            grid=(r // tile,),
            in_specs=[flat(d), flat(d)]
            + [specs[s](m.shape[-1]) for s, m in zip(mid_specs, mids)]
            + [pl.BlockSpec((1, d), lambda i, s: (0, 0))],
            out_specs=[flat(d)] * len(outs),
        ),
        out_shape=[jax.ShapeDtypeStruct((r, d), dt) for dt in outs],
        compiler_params=_params(32),
        cost_estimate=_cost(r * d * 3000, r * d * 16),
        name=name,
    )(ids, sa, sb, *mids, g)


def solution(mesh):
    def body(x, mu1, rs1, g1, g2, dy, wqkv, wo, w1, w2):
        hl, hd, d = wo.shape
        t = x.shape[0]
        b = t // NB
        r = b // 2
        me = lax.axis_index("tp")
        core, chip = me % 2, me // 2
        ids = jnp.stack([core, chip]).astype(jnp.int32)
        same = lambda v: lax.ppermute(v, "tp", SAME)
        cross = lambda v: lax.ppermute(v, "tp", CROSS)
        split = lambda v: v.reshape(NB, 2, r, v.shape[-1])
        pick = lambda v, c: lax.dynamic_index_in_dim(v, c, v.ndim - 3, keepdims=False)

        wo2 = wo.reshape(hl * hd, d)
        wo_cross = cross(wo2)
        wo_same = same(wo2)
        wo_diag = same(wo_cross)

        xf = x.astype(f32)
        n1 = ((xf - mu1[:, None]) * rs1[:, None] * g1.astype(f32)).astype(bf)
        qkv = _dot(n1, wqkv).astype(bf)

        o_own, o_same, o_cross, o_diag, lses, os = [], [], [], [], [], []
        npair = hl // 4
        for s in range(2):
            o, lse = _attn_fwd(qkv, hd, s * npair, npair)
            os.append(o)
            lses.append(lse)
            oc = cross(o)
            o_own.append(split(o))
            o_cross.append(split(oc))
            o_same.append(same(pick(split(o), 1 - core)))
            o_diag.append(same(pick(split(oc), 1 - core)))

        dg = _dot_t(dy, w2)

        xh2, rs2, n2_own, n2 = _h1(ids, split(x), o_own, o_same, o_cross, o_diag, (wo2, wo_same, wo_cross, wo_diag), g2[None])
        n2_other = same(n2_own)
        n2 = lax.dynamic_update_slice(n2, n2_other[:, None], (0, 1 - core, 0, 0)).reshape(t, d)

        a = _dot(n2, w1)
        gl, gelu_vjp = jax.vjp(jax.nn.gelu, a)
        gl = gl.astype(bf)
        da = gelu_vjp(dg)[0].astype(bf)
        da4 = da.reshape(NB, 2, r, da.shape[-1])

        part = _dot_t(pick(da4, 1 - core).reshape(NB * r, -1), w1).astype(bf)
        part = same(part).reshape(NB, r, d)
        da_own = pick(da4, core)

        dh = [None] * NB
        dhb = [None] * NB
        do = [None] * NB
        dhb_full = jnp.zeros((NB, 2, r, d), bf)
        sums = [None] * NB
        for k in reversed(range(NB)):
            s_own = (_dot_t(da_own[k], w1) + part[k].astype(f32)).astype(bf)
            sums[k] = (s_own, cross(s_own))

        acc = full = None
        dx = jnp.zeros((NB, 2, r, d), bf)
        x4, dy4 = split(x), split(dy)
        mu4, rs4 = mu1.reshape(NB, 2, 1, r), rs1.reshape(NB, 2, 1, r)
        w_t = wqkv
        for k in reversed(range(NB)):
            dh[k], dhb_own = _lnb(_lnb2_kernel, ids, *sums[k], (xh2, rs2, dy4), ("row", "row", "own"), g2[None], (f32, bf), f"lnb2_{k}", k)
            dhb_other = same(dhb_own)
            dhb_full = lax.dynamic_update_slice(dhb_full, dhb_own[None, None], (k, core, 0, 0))
            dhb_full = lax.dynamic_update_slice(dhb_full, dhb_other[None, None], (k, 1 - core, 0, 0))
            dhb[k] = jnp.where(core == 0, jnp.stack([dhb_own, dhb_other]), jnp.stack([dhb_other, dhb_own])).reshape(b, d)
            do[k] = _dot_t(dhb[k], wo2).astype(bf)
            res = _attn_bwd(qkv, os[0], os[1], do[k], lses[0], lses[1], acc, full, k, b, hd)
            dqkv_k, full = res[:2]
            acc = res[2] if k else None
            dq2 = dqkv_k.reshape(2, r, -1)
            p_other = same(_dot_t(pick(dq2, 1 - core), w_t).astype(bf))
            s_own = (_dot_t(pick(dq2, core), w_t) + p_other.astype(f32)).astype(bf)
            s_cross = cross(s_own)
            (dx_own,) = _lnb(_lnb1_kernel, ids, s_own, s_cross, (x4, mu4, rs4, dh[k]), ("own", "stat", "stat", "flat"), g1[None], (bf,), f"lnb1_{k}", k)
            dx_other = same(dx_own)
            dx = lax.dynamic_update_slice(dx, dx_own[None, None], (k, core, 0, 0))
            dx = lax.dynamic_update_slice(dx, dx_other[None, None], (k, 1 - core, 0, 0))

        dhb_all = dhb_full.reshape(t, d)
        dw2 = _dot(gl.T, dy).astype(bf)
        dw1 = _dot(n2.T, da).astype(bf)
        dwo = _dot(jnp.concatenate(os, 1).T, dhb_all).astype(bf).reshape(hl, hd, d)
        dwqkv = _dot(n1.T, full).astype(bf)
        return dx.reshape(t, d), dwqkv, dwo, dw1, dw2

    return jax.shard_map(
        body, mesh=mesh,
        in_specs=(P("dp", None), P("dp"), P("dp"), P(None), P(None), P("dp", None),
                  P(None, "tp"), P("tp", None, None), P(None, "tp"), P("tp", None)),
        out_specs=(P("dp", None), P("dp", "tp"), P(("dp", "tp"), None, None), P("dp", "tp"), P(("dp", "tp"), None)),
        check_vma=False)
```

```python
import functools

import jax
import jax.numpy as jnp
from jax import lax
from jax.experimental import pallas as pl
from jax.experimental.pallas import tpu as pltpu
from jax.sharding import PartitionSpec as P


EPS = 1.0 / 100000
LOG2E = 1.4426950408889634
f32 = jnp.float32
bf = jnp.bfloat16
NB = 2
BQ = 256
TILE = 256
MB = 2**20
SAME = [(0, 1), (1, 0), (2, 3), (3, 2)]
CROSS = [(0, 2), (2, 0), (1, 3), (3, 1)]


def _dot(a, b):
    return jnp.dot(a, b, preferred_element_type=f32)


def _dot_t(a, b):
    return lax.dot_general(a, b, (((1,), (1,)), ((), ())), preferred_element_type=f32)


def _causal(n):
    return lax.broadcasted_iota(jnp.int32, (n, n), 0) >= lax.broadcasted_iota(jnp.int32, (n, n), 1)


def _params(mb=60):
    return pltpu.CompilerParams(vmem_limit_bytes=mb * MB)


def _cost(flops, nbytes):
    return pl.CostEstimate(flops=int(flops), bytes_accessed=int(nbytes), transcendentals=0)


def _fwd_kernel(*refs, t, hd, first):
    qkv_ref = refs[0]
    o_ref, ofull_ref, lse_ref, tr_ref = refs[1:] if first else refs[4:]
    c = LOG2E * hd**-0.5
    for i in range(t // BQ):
        w = (i + 1) * BQ
        rows = slice(i * BQ, w)
        blk = qkv_ref[rows, :]
        tr_ref[0, :, rows] = blk.T
        scores = []
        for h in range(2):
            q = blk[:, 3 * hd * h : 3 * hd * h + hd]
            kt = slice(3 * hd * h + hd, 3 * hd * h + 2 * hd)
            s = _dot(q, tr_ref[0, kt, :w])
            d = jnp.where(_causal(BQ), s[:, w - BQ :], -jnp.inf)
            scores.append(jnp.concatenate([s[:, : w - BQ], d], 1) if i else d)
        cols, ps = [], []
        for s in scores:
            m = jnp.max(s, axis=1, keepdims=True)
            p = jnp.exp2((s - m) * c)
            l = jnp.sum(p, axis=1, keepdims=True)
            cols += [m * c + jnp.log2(l), 1.0 / l]
            ps.append(p.astype(bf))
        st = jnp.concatenate(cols, 1).T
        outs = []
        for h in range(2):
            vt = slice(3 * hd * h + 2 * hd, 3 * hd * h + 3 * hd)
            outs.append((_dot_t(tr_ref[0, vt, :w], ps[h]) * st[2 * h + 1 : 2 * h + 2]).astype(bf))
            lse_ref[0, h : h + 1, rows] = st[2 * h : 2 * h + 1]
        o = jnp.concatenate(outs, 0).T
        o_ref[rows, :] = o
        ofull_ref[rows, :] = o


def _attn_fwd(qkv, hd, start, npair, prev):
    t, w = qkv.shape
    total = w // (6 * hd)
    full = [jax.ShapeDtypeStruct((t, total * 2 * hd), bf), jax.ShapeDtypeStruct((total, 2, t), f32), jax.ShapeDtypeStruct((total, 6 * hd, t), bf)]
    return pl.pallas_call(
        functools.partial(_fwd_kernel, t=t, hd=hd, first=prev is None),
        grid=(npair,),
        in_specs=[pl.BlockSpec((t, 6 * hd), lambda p: (0, p + start))] + ([] if prev is None else [pl.BlockSpec(memory_space=pl.ANY)] * 3),
        out_specs=[
            pl.BlockSpec((t, 2 * hd), lambda p: (0, p)),
            pl.BlockSpec((t, 2 * hd), lambda p: (0, p + start)),
            pl.BlockSpec((1, 2, t), lambda p: (p + start, 0, 0)),
            pl.BlockSpec((1, 6 * hd, t), lambda p: (p + start, 0, 0)),
        ],
        out_shape=[jax.ShapeDtypeStruct((t, npair * 2 * hd), bf)] + full,
        input_output_aliases={} if prev is None else {1: 1, 2: 2, 3: 3},
        compiler_params=_params(),
        cost_estimate=_cost(npair * 9.5e9, npair * 2 * t * hd * 16),
        name="attn_fwd",
    )(qkv, *([] if prev is None else prev))


def _bwd_kernel(*refs, hd, r0, r1, has_in, has_out):
    qkv_ref, tr_ref, o_ref, do_ref, lse_ref = refs[:5]
    refs = refs[5:]
    acc_in = None
    if has_in:
        acc_in, _ = refs[:2]
        refs = refs[2:]
    out_ref, full_ref = refs[:2]
    refs = refs[2:]
    acc_out = None
    if has_out:
        acc_out = refs[0]
        refs = refs[1:]
    (g_t,) = refs
    sc = hd**-0.5
    c = LOG2E * sc
    if has_in:
        g_t[...] = acc_in[0]
    for i in reversed(range(r0 // BQ, r1 // BQ)):
        w = (i + 1) * BQ
        rows = slice(i * BQ, w)
        loc = slice(i * BQ - r0, w - r0)
        blk = qkv_ref[loc, 0 : 4 * hd]
        do2 = do_ref[loc, :]
        do_t = do2.T
        lse = lse_ref[0, :, rows].T
        prod = do2.astype(f32) * o_ref[loc, :].astype(f32)
        sd = []
        for h in range(2):
            b = 3 * hd * h
            s = _dot(blk[:, b : b + hd], tr_ref[0, b + hd : b + 2 * hd, :w])
            dp = _dot(do2[:, h * hd : (h + 1) * hd], tr_ref[0, b + 2 * hd : b + 3 * hd, :w])
            sd.append((s, dp))
        ew = []
        for h in range(2):
            s, dp = sd[h]
            p = jnp.exp2(s * c - lse[:, h : h + 1])
            d = jnp.where(_causal(BQ), p[:, w - BQ :], 0.0)
            p = jnp.concatenate([p[:, : w - BQ], d], 1) if i else d
            delta = jnp.sum(prod[:, h * hd : (h + 1) * hd], axis=1, keepdims=True)
            ew.append((p.astype(bf), (p * (dp - delta)).astype(bf)))
        outs = []
        for h in range(2):
            p, ds = ew[h]
            b = 3 * hd * h
            dv = _dot(do_t[h * hd : (h + 1) * hd], p)
            dk = _dot(tr_ref[0, b : b + hd, rows], ds)
            dq = _dot_t(tr_ref[0, b + hd : b + 2 * hd, :w], ds)
            kr = slice(2 * hd * h, 2 * hd * h + hd)
            vr = slice(2 * hd * h + hd, 2 * hd * h + 2 * hd)
            if w == r1 and not has_in:
                g_t[kr, :] = dk
                g_t[vr, :] = dv
            else:
                g_t[kr, :w] += dk
                g_t[vr, :w] += dv
            outs += [(dq * sc).astype(bf), (g_t[kr, rows] * sc).astype(bf), g_t[vr, rows].astype(bf)]
        res = jnp.concatenate(outs, 0).T
        out_ref[loc, :] = res
        full_ref[loc, :] = res
    if has_out:
        acc_out[0] = g_t[:, :r0]


def _attn_bwd(qkv, tr, o, do, lse, acc, full, chunk, b, hd):
    t, w = qkv.shape
    npair = w // (6 * hd)
    r0, r1 = chunk * b, (chunk + 1) * b
    has_in, has_out = acc is not None, r0 > 0
    in_specs = [
        pl.BlockSpec((b, 6 * hd), lambda p: (chunk, p)),
        pl.BlockSpec((1, 6 * hd, r1), lambda p: (p, 0, 0)),
        pl.BlockSpec((b, 2 * hd), lambda p: (chunk, p)),
        pl.BlockSpec((b, 2 * hd), lambda p: (0, p)),
        pl.BlockSpec((1, 2, t), lambda p: (p, 0, 0)),
    ]
    args = [qkv, tr, o, do, lse]
    alias = {}
    if has_in:
        in_specs += [pl.BlockSpec((1, 4 * hd, r1), lambda p: (p, 0, 0)), pl.BlockSpec(memory_space=pl.ANY)]
        args += [acc, full]
        alias = {6: 1}
    out_specs = [pl.BlockSpec((b, 6 * hd), lambda p: (0, p)), pl.BlockSpec((b, 6 * hd), lambda p: (chunk, p))]
    out_shape = [jax.ShapeDtypeStruct((b, w), bf), jax.ShapeDtypeStruct((t, w), bf)]
    if has_out:
        out_specs.append(pl.BlockSpec((1, 4 * hd, r0), lambda p: (p, 0, 0)))
        out_shape.append(jax.ShapeDtypeStruct((npair, 4 * hd, r0), f32))
    work = npair * 2 * b * (r0 + r1)
    return pl.pallas_call(
        functools.partial(_bwd_kernel, hd=hd, r0=r0, r1=r1, has_in=has_in, has_out=has_out),
        grid=(npair,),
        in_specs=in_specs,
        out_specs=out_specs,
        out_shape=out_shape,
        scratch_shapes=[pltpu.VMEM((4 * hd, r1), f32)],
        input_output_aliases=alias,
        compiler_params=_params(),
        cost_estimate=_cost(work * 1500, 3 * t * w),
    )(*args)


def _h1_kernel(ids, x_ref, oa, ob, pa, pb, qa, qb, ra, rb, wa, wb, wc, wd, g_ref, xh_ref, rs_ref, own_ref, full_ref, acc):
    def run(first, second):
        acc[...] = sum(_dot(jnp.concatenate([u, v], 1), w[...]) for u, v, w in first + second)

    near = [(oa[0, 0], ob[0, 0], wa), (pa[0], pb[0], wb)]
    far = [(qa[0, 0], qb[0, 0], wc), (ra[0], rb[0], wd)]

    @pl.when(ids[1] == 0)
    def _():
        run(near, far)

    @pl.when(ids[1] != 0)
    def _():
        run(far, near)

    h1 = x_ref[0, 0].astype(f32) + acc[...]
    xc = h1 - jnp.mean(h1, axis=1, keepdims=True)
    rs = lax.rsqrt(jnp.mean(xc * xc, axis=1, keepdims=True) + EPS)
    xh = xc * rs
    n2 = (xh * g_ref[...].astype(f32)).astype(bf)
    xh_ref[...] = xh
    rs_ref[...] = jnp.broadcast_to(rs, (rs.shape[0], 128))
    own_ref[...] = n2
    full_ref[0] = n2


def _h1(ids, chunk, x4, o_own, o_same, o_cross, o_diag, ws, g2):
    _, _, r, d = x4.shape
    own = lambda k: pl.BlockSpec((1, 1, TILE, k), lambda i, s: (chunk, s[0], i, 0))
    row = lambda k: pl.BlockSpec((1, TILE, k), lambda i, s: (chunk, i, 0))
    flat = lambda k: pl.BlockSpec((TILE, k), lambda i, s: (i, 0))
    const = lambda shape: pl.BlockSpec(shape, lambda i, s: (0, 0), pipeline_mode=pl.Buffered(1))
    k = o_own[0].shape[-1]
    return pl.pallas_call(
        _h1_kernel,
        grid_spec=pltpu.PrefetchScalarGridSpec(
            num_scalar_prefetch=1,
            grid=(r // TILE,),
            in_specs=[own(d), own(k), own(k), row(k), row(k), own(k), own(k), row(k), row(k)]
            + [const((2 * k, d))] * 4
            + [const((1, d))],
            out_specs=[flat(d), flat(128), flat(d), pl.BlockSpec((1, TILE, d), lambda i, s: (s[0], i, 0))],
            scratch_shapes=[pltpu.VMEM((TILE, d), f32)],
        ),
        out_shape=[
            jax.ShapeDtypeStruct((r, d), f32),
            jax.ShapeDtypeStruct((r, 128), f32),
            jax.ShapeDtypeStruct((r, d), bf),
            jax.ShapeDtypeStruct((2, r, d), bf),
        ],
        compiler_params=_params(),
        cost_estimate=_cost(2 * r * d * 8 * k, 20 * MB),
    )(ids, x4, *o_own, *o_same, *o_cross, *o_diag, *ws, g2)


def _place_kernel(ids, v_ref, _, buf_ref):
    buf_ref[0] = v_ref[...]


def _place(ids, buf, v):
    r, d = v.shape
    return pl.pallas_call(
        _place_kernel,
        grid_spec=pltpu.PrefetchScalarGridSpec(
            num_scalar_prefetch=1,
            grid=(r // TILE,),
            in_specs=[pl.BlockSpec((TILE, d), lambda i, s: (i, 0)), pl.BlockSpec(memory_space=pl.ANY)],
            out_specs=pl.BlockSpec((1, TILE, d), lambda i, s: (1 - s[0], i, 0)),
        ),
        out_shape=jax.ShapeDtypeStruct(buf.shape, buf.dtype),
        input_output_aliases={2: 0},
        compiler_params=_params(32),
        cost_estimate=_cost(r * d * 1000, 2 * r * d * 2),
    )(ids, v, buf)


def _place4_kernel(ids, v_ref, _, buf_ref):
    buf_ref[0, 0] = v_ref[...]


def _place4(ids, buf, v, chunk):
    r, d = v.shape
    return pl.pallas_call(
        _place4_kernel,
        grid_spec=pltpu.PrefetchScalarGridSpec(
            num_scalar_prefetch=1,
            grid=(r // TILE,),
            in_specs=[pl.BlockSpec((TILE, d), lambda i, s: (i, 0)), pl.BlockSpec(memory_space=pl.ANY)],
            out_specs=pl.BlockSpec((1, 1, TILE, d), lambda i, s: (chunk, 1 - s[0], i, 0)),
        ),
        out_shape=jax.ShapeDtypeStruct(buf.shape, buf.dtype),
        input_output_aliases={2: 0},
        compiler_params=_params(32),
        cost_estimate=_cost(r * d * 1000, 2 * r * d * 2),
    )(ids, v, buf)


def _lnb2_kernel(ids, sa, sb, xh_ref, rs_ref, dy_ref, g_ref, dh_ref, own_ref, full_ref):
    u = (sa[...].astype(f32) + sb[...].astype(f32)) * g_ref[...].astype(f32)
    xh = xh_ref[...]
    v = u - jnp.mean(u, axis=1, keepdims=True) - xh * jnp.mean(u * xh, axis=1, keepdims=True)
    dh = dy_ref[0, 0].astype(f32) + rs_ref[:, :1] * v
    dhb = dh.astype(bf)
    dh_ref[...] = dh
    own_ref[...] = dhb
    full_ref[0] = dhb


def _lnb1_kernel(ids, sa, sb, x_ref, mu_ref, rs_ref, dh_ref, g_ref, *outs):
    u = (sa[...].astype(f32) + sb[...].astype(f32)) * g_ref[...].astype(f32)
    rs = rs_ref[0, 0].T
    xh = (x_ref[0, 0].astype(f32) - mu_ref[0, 0].T) * rs
    v = u - jnp.mean(u, axis=1, keepdims=True) - xh * jnp.mean(u * xh, axis=1, keepdims=True)
    dx = (dh_ref[...] + rs * v).astype(bf)
    outs[-2][...] = dx
    outs[-1][0, 0] = dx


def _lnb(kernel, ids, chunk, args, kinds, outs, out_kinds, alias=None, tile=128):
    r = args[0].shape[0]
    specs = {
        "flat": lambda k: pl.BlockSpec((tile, k), lambda i, s: (i, 0)),
        "own": lambda k: pl.BlockSpec((1, 1, tile, k), lambda i, s: (chunk, s[0], i, 0)),
        "stat": lambda k: pl.BlockSpec((1, 1, 1, tile), lambda i, s: (chunk, s[0], 0, i)),
        "gain": lambda k: pl.BlockSpec((1, k), lambda i, s: (0, 0)),
        "pair": lambda k: pl.BlockSpec((1, tile, k), lambda i, s: (s[0], i, 0)),
        "any": lambda k: pl.BlockSpec(memory_space=pl.ANY),
    }
    return pl.pallas_call(
        kernel,
        grid_spec=pltpu.PrefetchScalarGridSpec(
            num_scalar_prefetch=1,
            grid=(r // tile,),
            in_specs=[specs[k](a.shape[-1]) for k, a in zip(kinds, args)],
            out_specs=[specs[k](o.shape[-1]) for k, o in zip(out_kinds, outs)],
        ),
        out_shape=outs,
        input_output_aliases=alias or {},
        compiler_params=_params(32),
        cost_estimate=_cost(r * 2048 * 6000, r * 2048 * 16),
    )(ids, *args)


class _Chain:
    def __init__(self):
        self.last = None

    def tie(self, *args):
        if self.last is not None:
            *args, _ = lax.optimization_barrier((*args, self.last))
        return args if len(args) > 1 else args[0]

    def did(self, v):
        self.last = v
        return v


def solution(mesh):
    def body(x, mu1, rs1, g1, g2, dy, wqkv, wo, w1, w2):
        hl, hd, d = wo.shape
        t = x.shape[0]
        b = t // NB
        r = b // 2
        me = lax.axis_index("tp")
        core, chip = me % 2, me // 2
        ids = jnp.stack([core, chip]).astype(jnp.int32)

        def same(v):
            return lax.ppermute(v, "tp", SAME)

        def cross(v):
            return lax.ppermute(v, "tp", CROSS)

        split = lambda v: v.reshape(NB, 2, r, v.shape[-1])
        pick = lambda v, c: lax.dynamic_index_in_dim(v, c, v.ndim - 3, keepdims=False)
        sds = jax.ShapeDtypeStruct
        order = _Chain()
        tie, did = order.tie, order.did
        chunks = list(reversed(range(NB)))

        wo2 = wo.reshape(hl * hd, d)
        wo_cross = cross(wo2)
        wo_same = same(wo2)
        wo_diag = same(wo_cross)

        xf = x.astype(f32)
        n1 = ((xf - mu1[:, None]) * rs1[:, None] * g1.astype(f32)).astype(bf)
        qkv = did(_dot(n1, wqkv).astype(bf))

        o_own, o_same, o_cross, o_diag = [], [], [], []
        npair = hl // 4
        prev = None
        for s in range(2):
            o, *prev = _attn_fwd(tie(qkv), hd, s * npair, npair, prev)
            did(o)
            oc = cross(o)
            o_own.append(split(o))
            o_cross.append(split(oc))
            o_same.append(same(pick(split(o), 1 - core)))
            o_diag.append(same(pick(split(oc), 1 - core)))
        o_all, lse, qkv_t = prev

        dg = did(_dot_t(tie(dy), w2))

        x4, dy4 = split(x), split(dy)
        xh2, rs2, n2, others = [None] * NB, [None] * NB, [None] * NB, [None] * NB
        for k in chunks:
            xh2[k], rs2[k], own, n2[k] = _h1(
                ids, k, tie(x4), o_own, o_same, o_cross, o_diag, (wo2, wo_same, wo_cross, wo_diag), g2[None]
            )
            did(own)
            others[k] = same(own)

        gl, da, sums, n2f = [None] * NB, [None] * NB, [None] * NB, [None] * NB
        dyc = dy.reshape(NB, b, d)
        dgc = dg.reshape(NB, b, -1)

        def place_n2(k):
            n2f[k] = did(_place(ids, tie(n2[k]), others[k])).reshape(b, d)

        def mlp(k):
            a = _dot(tie(n2f[k]), w1)
            g, gelu_vjp = jax.vjp(jax.nn.gelu, a)
            gl[k] = g.astype(bf)
            da[k] = did(gelu_vjp(dgc[k])[0].astype(bf))

        def partial_other(v, w):
            p = did(_dot_t(pick(tie(v).reshape(2, r, -1), 1 - core), w).astype(bf))
            return same(p)

        def partial_own(v, w, recv):
            s_own = did((_dot_t(pick(tie(v).reshape(2, r, -1), core), w) + recv.astype(f32)).astype(bf))
            return s_own, cross(s_own)

        def grad(u, v, add=None, keep=False):
            p = _dot(tie(u).T, v)
            p = p if add is None else p + add
            return did(p if keep else p.astype(bf))

        place_n2(1)
        mlp(1)
        recv = partial_other(da[1], w1)
        place_n2(0)
        sums[1] = partial_own(da[1], w1, recv)
        mlp(0)
        recv = partial_other(da[0], w1)
        dw2 = grad(gl[1], dyc[1], keep=True)
        sums[0] = partial_own(da[0], w1, recv)

        dh, dhb = [None] * NB, [None] * NB

        def norm2(k):
            dh[k], own, dhb[k] = _lnb(
                _lnb2_kernel, ids, k, (tie(sums[k][0]), sums[k][1], xh2[k], rs2[k], dy4, g2[None]),
                ("flat", "flat", "flat", "flat", "own", "gain"),
                (sds((r, d), f32), sds((r, d), bf), sds((2, r, d), bf)), ("flat", "flat", "pair"),
            )
            did(own)
            return same(own)

        def attention(k, other, acc, full):
            dhb[k] = did(_place(ids, tie(dhb[k]), other)).reshape(b, d)
            do = did(_dot_t(tie(dhb[k]), wo2).astype(bf))
            res = _attn_bwd(qkv, qkv_t, o_all, do, lse, acc, full, k, b, hd)
            did(res[0])
            return res

        def norm1(k, pair, dx):
            args = (tie(pair[0]), pair[1], x4, mu4, rs4, dh[k], g1[None]) + (() if dx is None else (dx,))
            own, dx = _lnb(
                _lnb1_kernel, ids, k, args, ("flat", "flat", "own", "stat", "stat", "flat", "gain", "any")[: len(args)],
                (sds((r, d), bf), sds((NB, 2, r, d), bf)), ("flat", "own"),
                None if dx is None else {8: 1},
            )
            did(own)
            return same(own), dx

        mu4, rs4 = mu1.reshape(NB, 2, 1, r), rs1.reshape(NB, 2, 1, r)
        o3 = o_all.reshape(NB, b, -1)

        other = norm2(1)
        dw2 = grad(gl[0], dyc[0], dw2)
        dq1, full, acc = attention(1, other, None, None)
        recv = partial_other(dq1, wqkv)
        other = norm2(0)
        pair1 = partial_own(dq1, wqkv, recv)
        dq0, full = attention(0, other, acc, full)
        recv = partial_other(dq0, wqkv)
        dwo = grad(o3[1], dhb[1], keep=True)
        pair0 = partial_own(dq0, wqkv, recv)
        dwo = grad(o3[0], dhb[0], dwo).reshape(hl, hd, d)
        dw1 = grad(n2f[1], da[1], keep=True)
        dw1 = grad(n2f[0], da[0], dw1)
        other1, dx = norm1(1, pair1, None)
        dwqkv = grad(n1, full)
        other0, dx = norm1(0, pair0, dx)
        dx = _place4(ids, dx, other1, 1)
        dx = _place4(ids, dx, other0, 0)
        return dx.reshape(t, d), dwqkv, dwo, dw1, dw2

    return jax.shard_map(
        body, mesh=mesh,
        in_specs=(P("dp", None), P("dp"), P("dp"), P(None), P(None), P("dp", None),
                  P(None, "tp"), P("tp", None, None), P(None, "tp"), P("tp", None)),
        out_specs=(P("dp", None), P("dp", "tp"), P(("dp", "tp"), None, None), P("dp", "tp"), P(("dp", "tp"), None)),
        check_vma=False)
```

```python
import functools

import jax
import jax.numpy as jnp
from jax import lax
from jax.experimental import pallas as pl
from jax.experimental.pallas import tpu as pltpu
from jax.sharding import PartitionSpec as P


EPS = 1.0 / 100000
LOG2E = 1.4426950408889634
f32 = jnp.float32
bf = jnp.bfloat16
NB = 2
BQ = 256
TILE = 256
MB = 2**20
SAME = [(0, 1), (1, 0), (2, 3), (3, 2)]
CROSS = [(0, 2), (2, 0), (1, 3), (3, 1)]


def _dot(a, b):
    return jnp.dot(a, b, preferred_element_type=f32)


def _dot_t(a, b):
    return lax.dot_general(a, b, (((1,), (1,)), ((), ())), preferred_element_type=f32)


def _causal(n):
    return lax.broadcasted_iota(jnp.int32, (n, n), 0) >= lax.broadcasted_iota(jnp.int32, (n, n), 1)


def _params(mb=60):
    return pltpu.CompilerParams(vmem_limit_bytes=mb * MB)


def _cost(flops, nbytes):
    return pl.CostEstimate(flops=int(flops), bytes_accessed=int(nbytes), transcendentals=0)


def _fwd_kernel(*refs, t, hd, first):
    qkv_ref = refs[0]
    o_ref, ofull_ref, lse_ref, tr_ref = refs[1:] if first else refs[4:]
    c = LOG2E * hd**-0.5
    for i in range(t // BQ):
        w = (i + 1) * BQ
        rows = slice(i * BQ, w)
        blk = qkv_ref[rows, :]
        tr_ref[0, :, rows] = blk.T
        scores = []
        for h in range(2):
            q = blk[:, 3 * hd * h : 3 * hd * h + hd]
            kt = slice(3 * hd * h + hd, 3 * hd * h + 2 * hd)
            s = _dot(q, tr_ref[0, kt, :w])
            d = jnp.where(_causal(BQ), s[:, w - BQ :], -jnp.inf)
            scores.append(jnp.concatenate([s[:, : w - BQ], d], 1) if i else d)
        cols, ps = [], []
        for s in scores:
            m = jnp.max(s, axis=1, keepdims=True)
            p = jnp.exp2((s - m) * c)
            l = jnp.sum(p, axis=1, keepdims=True)
            cols += [m * c + jnp.log2(l), 1.0 / l]
            ps.append(p.astype(bf))
        st = jnp.concatenate(cols, 1).T
        outs = []
        for h in range(2):
            vt = slice(3 * hd * h + 2 * hd, 3 * hd * h + 3 * hd)
            outs.append((_dot_t(tr_ref[0, vt, :w], ps[h]) * st[2 * h + 1 : 2 * h + 2]).astype(bf))
            lse_ref[0, h : h + 1, rows] = st[2 * h : 2 * h + 1]
        o = jnp.concatenate(outs, 0).T
        o_ref[rows, :] = o
        ofull_ref[rows, :] = o


def _attn_fwd(qkv, hd, start, npair, prev):
    t, w = qkv.shape
    total = w // (6 * hd)
    full = [jax.ShapeDtypeStruct((t, total * 2 * hd), bf), jax.ShapeDtypeStruct((total, 2, t), f32), jax.ShapeDtypeStruct((total, 6 * hd, t), bf)]
    return pl.pallas_call(
        functools.partial(_fwd_kernel, t=t, hd=hd, first=prev is None),
        grid=(npair,),
        in_specs=[pl.BlockSpec((t, 6 * hd), lambda p: (0, p + start))] + ([] if prev is None else [pl.BlockSpec(memory_space=pl.ANY)] * 3),
        out_specs=[
            pl.BlockSpec((t, 2 * hd), lambda p: (0, p)),
            pl.BlockSpec((t, 2 * hd), lambda p: (0, p + start)),
            pl.BlockSpec((1, 2, t), lambda p: (p + start, 0, 0)),
            pl.BlockSpec((1, 6 * hd, t), lambda p: (p + start, 0, 0)),
        ],
        out_shape=[jax.ShapeDtypeStruct((t, npair * 2 * hd), bf)] + full,
        input_output_aliases={} if prev is None else {1: 1, 2: 2, 3: 3},
        compiler_params=_params(),
        cost_estimate=_cost(npair * 9.5e9, npair * 2 * t * hd * 16),
        name="attn_fwd",
    )(qkv, *([] if prev is None else prev))


def _bwd_kernel(*refs, hd, r0, r1, has_in, has_out):
    ids, qkv_ref, tr_ref, o_ref, do_ref, lse_ref = refs[:6]
    refs = refs[6:]
    acc_in = None
    if has_in:
        acc_in, _ = refs[:2]
        refs = refs[2:]
    own_ref, other_ref, full_ref = refs[:3]
    refs = refs[3:]
    acc_out = None
    if has_out:
        acc_out = refs[0]
        refs = refs[1:]
    (g_t,) = refs
    sc = hd**-0.5
    c = LOG2E * sc
    if has_in:
        g_t[...] = acc_in[0]
    for i in reversed(range(r0 // BQ, r1 // BQ)):
        w = (i + 1) * BQ
        rows = slice(i * BQ, w)
        loc = slice(i * BQ - r0, w - r0)
        blk = qkv_ref[loc, 0 : 4 * hd]
        do2 = do_ref[loc, :]
        do_t = do2.T
        lse = lse_ref[0, :, rows].T
        prod = do2.astype(f32) * o_ref[loc, :].astype(f32)
        sd = []
        for h in range(2):
            b = 3 * hd * h
            s = _dot(blk[:, b : b + hd], tr_ref[0, b + hd : b + 2 * hd, :w])
            dp = _dot(do2[:, h * hd : (h + 1) * hd], tr_ref[0, b + 2 * hd : b + 3 * hd, :w])
            sd.append((s, dp))
        ew = []
        for h in range(2):
            s, dp = sd[h]
            p = jnp.exp2(s * c - lse[:, h : h + 1])
            d = jnp.where(_causal(BQ), p[:, w - BQ :], 0.0)
            p = jnp.concatenate([p[:, : w - BQ], d], 1) if i else d
            delta = jnp.sum(prod[:, h * hd : (h + 1) * hd], axis=1, keepdims=True)
            ew.append((p.astype(bf), (p * (dp - delta)).astype(bf)))
        outs = []
        for h in range(2):
            p, ds = ew[h]
            b = 3 * hd * h
            dv = _dot(do_t[h * hd : (h + 1) * hd], p)
            dk = _dot(tr_ref[0, b : b + hd, rows], ds)
            dq = _dot_t(tr_ref[0, b + hd : b + 2 * hd, :w], ds)
            kr = slice(2 * hd * h, 2 * hd * h + hd)
            vr = slice(2 * hd * h + hd, 2 * hd * h + 2 * hd)
            if w == r1 and not has_in:
                g_t[kr, :] = dk
                g_t[vr, :] = dv
            else:
                g_t[kr, :w] += dk
                g_t[vr, :w] += dv
            outs += [(dq * sc).astype(bf), (g_t[kr, rows] * sc).astype(bf), g_t[vr, rows].astype(bf)]
        full_ref[loc, :] = jnp.concatenate(outs, 0).T
    half = (r1 - r0) // 2
    own_ref[...] = full_ref[pl.ds(pl.multiple_of(ids[0] * half, half), half), :]
    other_ref[...] = full_ref[pl.ds(pl.multiple_of((1 - ids[0]) * half, half), half), :]
    if has_out:
        acc_out[0] = g_t[:, :r0]


def _attn_bwd(ids, qkv, tr, o, do, lse, acc, full, chunk, b, hd):
    t, w = qkv.shape
    npair = w // (6 * hd)
    r0, r1 = chunk * b, (chunk + 1) * b
    has_in, has_out = acc is not None, r0 > 0
    in_specs = [
        pl.BlockSpec((b, 6 * hd), lambda p, s: (chunk, p)),
        pl.BlockSpec((1, 6 * hd, r1), lambda p, s: (p, 0, 0)),
        pl.BlockSpec((b, 2 * hd), lambda p, s: (chunk, p)),
        pl.BlockSpec((b, 2 * hd), lambda p, s: (0, p)),
        pl.BlockSpec((1, 2, t), lambda p, s: (p, 0, 0)),
    ]
    args = [qkv, tr, o, do, lse]
    alias = {}
    if has_in:
        in_specs += [pl.BlockSpec((1, 4 * hd, r1), lambda p, s: (p, 0, 0)), pl.BlockSpec(memory_space=pl.ANY)]
        args += [acc, full]
        alias = {7: 2}
    out_specs = [pl.BlockSpec((b // 2, 6 * hd), lambda p, s: (0, p))] * 2 + [pl.BlockSpec((b, 6 * hd), lambda p, s: (chunk, p))]
    out_shape = [jax.ShapeDtypeStruct((b // 2, w), bf)] * 2 + [jax.ShapeDtypeStruct((t, w), bf)]
    if has_out:
        out_specs.append(pl.BlockSpec((1, 4 * hd, r0), lambda p, s: (p, 0, 0)))
        out_shape.append(jax.ShapeDtypeStruct((npair, 4 * hd, r0), f32))
    work = npair * 2 * b * (r0 + r1)
    return pl.pallas_call(
        functools.partial(_bwd_kernel, hd=hd, r0=r0, r1=r1, has_in=has_in, has_out=has_out),
        grid_spec=pltpu.PrefetchScalarGridSpec(
            num_scalar_prefetch=1,
            grid=(npair,),
            in_specs=in_specs,
            out_specs=out_specs,
            scratch_shapes=[pltpu.VMEM((4 * hd, r1), f32)],
        ),
        out_shape=out_shape,
        input_output_aliases=alias,
        compiler_params=_params(),
        cost_estimate=_cost(work * 1500, 3 * t * w),
    )(ids, *args)


def _h1_kernel(ids, x_ref, oa, ob, pa, pb, qa, qb, ra, rb, wa, wb, wc, wd, g_ref, xh_ref, rs_ref, own_ref, full_ref, acc):
    def run(first, second):
        acc[...] = sum(_dot(jnp.concatenate([u, v], 1), w[...]) for u, v, w in first + second)

    near = [(oa[0, 0], ob[0, 0], wa), (pa[0, 0], pb[0, 0], wb)]
    far = [(qa[0, 0], qb[0, 0], wc), (ra[0, 0], rb[0, 0], wd)]

    @pl.when(ids[1] == 0)
    def _():
        run(near, far)

    @pl.when(ids[1] != 0)
    def _():
        run(far, near)

    h1 = x_ref[0, 0].astype(f32) + acc[...]
    xc = h1 - jnp.mean(h1, axis=1, keepdims=True)
    rs = lax.rsqrt(jnp.mean(xc * xc, axis=1, keepdims=True) + EPS)
    xh = xc * rs
    n2 = (xh * g_ref[...].astype(f32)).astype(bf)
    xh_ref[...] = xh
    rs_ref[...] = jnp.broadcast_to(rs, (rs.shape[0], 128))
    own_ref[...] = n2
    full_ref[0] = n2


def _h1(ids, chunk, x4, o_own, o_same, o_cross, o_diag, ws, g2):
    _, _, r, d = x4.shape
    own = lambda k: pl.BlockSpec((1, 1, TILE, k), lambda i, s: (chunk, s[0], i, 0))
    flat = lambda k: pl.BlockSpec((TILE, k), lambda i, s: (i, 0))
    const = lambda shape: pl.BlockSpec(shape, lambda i, s: (0, 0), pipeline_mode=pl.Buffered(1))
    k = o_own[0].shape[-1]
    return pl.pallas_call(
        _h1_kernel,
        grid_spec=pltpu.PrefetchScalarGridSpec(
            num_scalar_prefetch=1,
            grid=(r // TILE,),
            in_specs=[own(d)] + [own(k)] * 8
            + [const((2 * k, d))] * 4
            + [const((1, d))],
            out_specs=[flat(d), flat(128), flat(d), pl.BlockSpec((1, TILE, d), lambda i, s: (s[0], i, 0))],
            scratch_shapes=[pltpu.VMEM((TILE, d), f32)],
        ),
        out_shape=[
            jax.ShapeDtypeStruct((r, d), f32),
            jax.ShapeDtypeStruct((r, 128), f32),
            jax.ShapeDtypeStruct((r, d), bf),
            jax.ShapeDtypeStruct((2, r, d), bf),
        ],
        compiler_params=_params(),
        cost_estimate=_cost(2 * r * d * 8 * k, 20 * MB),
    )(ids, x4, *o_own, *o_same, *o_cross, *o_diag, *ws, g2)


GC0 = 0.7978845608028654
GC1 = 0.044715


def _mlp_kernel(ids, n_ref, w_ref, dg_ref, *refs):
    gl_ref, da_ref, own_ref, other_ref = refs[-4:]
    sub = own_ref.shape[0]
    for half in range(2):
        rows = slice(half * sub, half * sub + sub)
        a = _dot(n_ref[rows, :], w_ref[...])
        a2 = a * a
        h = 0.5 + 0.5 * jnp.tanh(a * (GC0 + GC0 * GC1 * a2))
        gl_ref[rows, :] = (a * h).astype(bf)
        slope = h + a * (2.0 * h * (1.0 - h)) * (GC0 + 3.0 * GC0 * GC1 * a2)
        da_ref[rows, :] = (dg_ref[rows, :] * slope).astype(bf)
    own_ref[...] = da_ref[pl.ds(pl.multiple_of(ids[0] * sub, sub), sub), :]
    other_ref[...] = da_ref[pl.ds(pl.multiple_of((1 - ids[0]) * sub, sub), sub), :]


def _mlp(ids, n2, w1, dg, chunk, prev, bn=512):
    b, d = n2.shape
    t, f = dg.shape
    spec = pl.BlockSpec((b, bn), lambda j, s: (chunk, j))
    half = pl.BlockSpec((b // 2, bn), lambda j, s: (0, j))
    return pl.pallas_call(
        _mlp_kernel,
        grid_spec=pltpu.PrefetchScalarGridSpec(
            num_scalar_prefetch=1,
            grid=(f // bn,),
            in_specs=[
                pl.BlockSpec((b, d), lambda j, s: (0, 0), pipeline_mode=pl.Buffered(1)),
                pl.BlockSpec((d, bn), lambda j, s: (0, j)),
                spec,
            ]
            + [pl.BlockSpec(memory_space=pl.ANY)] * len(prev),
            out_specs=[spec, spec, half, half],
        ),
        out_shape=[jax.ShapeDtypeStruct((t, f), bf)] * 2 + [jax.ShapeDtypeStruct((b // 2, f), bf)] * 2,
        input_output_aliases={4: 0, 5: 1} if prev else {},
        compiler_params=_params(),
        cost_estimate=_cost(2 * b * d * f * 1.3, 2 * b * f * 8),
    )(ids, n2, w1, dg, *prev)


def _place_kernel(ids, v_ref, _, buf_ref):
    buf_ref[0] = v_ref[...]


def _place(ids, buf, v):
    r, d = v.shape
    return pl.pallas_call(
        _place_kernel,
        grid_spec=pltpu.PrefetchScalarGridSpec(
            num_scalar_prefetch=1,
            grid=(r // TILE,),
            in_specs=[pl.BlockSpec((TILE, d), lambda i, s: (i, 0)), pl.BlockSpec(memory_space=pl.ANY)],
            out_specs=pl.BlockSpec((1, TILE, d), lambda i, s: (1 - s[0], i, 0)),
        ),
        out_shape=jax.ShapeDtypeStruct(buf.shape, buf.dtype),
        input_output_aliases={2: 0},
        compiler_params=_params(),
        cost_estimate=_cost(r * d * 1000, 2 * r * d * 2),
    )(ids, v, buf)


def _place4_kernel(ids, v_ref, _, buf_ref):
    buf_ref[0, 0] = v_ref[...]


def _place4(ids, buf, v, chunk):
    r, d = v.shape
    return pl.pallas_call(
        _place4_kernel,
        grid_spec=pltpu.PrefetchScalarGridSpec(
            num_scalar_prefetch=1,
            grid=(r // TILE,),
            in_specs=[pl.BlockSpec((TILE, d), lambda i, s: (i, 0)), pl.BlockSpec(memory_space=pl.ANY)],
            out_specs=pl.BlockSpec((1, 1, TILE, d), lambda i, s: (chunk, 1 - s[0], i, 0)),
        ),
        out_shape=jax.ShapeDtypeStruct(buf.shape, buf.dtype),
        input_output_aliases={2: 0},
        compiler_params=_params(),
        cost_estimate=_cost(r * d * 1000, 2 * r * d * 2),
    )(ids, v, buf)


def _lnb2_kernel(ids, sa, sb, xh_ref, rs_ref, dy_ref, g_ref, dh_ref, own_ref, full_ref):
    u = (sa[...].astype(f32) + sb[...].astype(f32)) * g_ref[...].astype(f32)
    xh = xh_ref[...]
    v = u - jnp.mean(u, axis=1, keepdims=True) - xh * jnp.mean(u * xh, axis=1, keepdims=True)
    dh = dy_ref[0, 0].astype(f32) + rs_ref[:, :1] * v
    dhb = dh.astype(bf)
    dh_ref[...] = dh
    own_ref[...] = dhb
    full_ref[0] = dhb


def _lnb1_kernel(ids, sa, sb, x_ref, mu_ref, rs_ref, dh_ref, g_ref, *outs):
    u = (sa[...].astype(f32) + sb[...].astype(f32)) * g_ref[...].astype(f32)
    rs = rs_ref[0, 0].T
    xh = (x_ref[0, 0].astype(f32) - mu_ref[0, 0].T) * rs
    v = u - jnp.mean(u, axis=1, keepdims=True) - xh * jnp.mean(u * xh, axis=1, keepdims=True)
    dx = (dh_ref[...] + rs * v).astype(bf)
    outs[-2][...] = dx
    outs[-1][0, 0] = dx


def _lnb(kernel, ids, chunk, args, kinds, outs, out_kinds, alias=None, tile=128):
    r = args[0].shape[0]
    specs = {
        "flat": lambda k: pl.BlockSpec((tile, k), lambda i, s: (i, 0)),
        "own": lambda k: pl.BlockSpec((1, 1, tile, k), lambda i, s: (chunk, s[0], i, 0)),
        "stat": lambda k: pl.BlockSpec((1, 1, 1, tile), lambda i, s: (chunk, s[0], 0, i)),
        "gain": lambda k: pl.BlockSpec((1, k), lambda i, s: (0, 0)),
        "pair": lambda k: pl.BlockSpec((1, tile, k), lambda i, s: (s[0], i, 0)),
        "any": lambda k: pl.BlockSpec(memory_space=pl.ANY),
    }
    return pl.pallas_call(
        kernel,
        grid_spec=pltpu.PrefetchScalarGridSpec(
            num_scalar_prefetch=1,
            grid=(r // tile,),
            in_specs=[specs[k](a.shape[-1]) for k, a in zip(kinds, args)],
            out_specs=[specs[k](o.shape[-1]) for k, o in zip(out_kinds, outs)],
        ),
        out_shape=outs,
        input_output_aliases=alias or {},
        compiler_params=_params(),
        cost_estimate=_cost(r * 2048 * 6000, r * 2048 * 16),
    )(ids, *args)


class _Chain:
    def __init__(self):
        self.last = None

    def tie(self, *args):
        if self.last is not None:
            *args, _ = lax.optimization_barrier((*args, self.last))
        return args if len(args) > 1 else args[0]

    def did(self, v):
        self.last = v
        return v


def solution(mesh):
    def body(x, mu1, rs1, g1, g2, dy, wqkv, wo, w1, w2):
        hl, hd, d = wo.shape
        t = x.shape[0]
        b = t // NB
        r = b // 2
        me = lax.axis_index("tp")
        core, chip = me % 2, me // 2
        ids = jnp.stack([core, chip]).astype(jnp.int32)

        def same(v):
            return lax.ppermute(v, "tp", SAME)

        def cross(v):
            return lax.ppermute(v, "tp", CROSS)

        split = lambda v: v.reshape(NB, 2, r, v.shape[-1])
        sds = jax.ShapeDtypeStruct
        order = _Chain()
        tie, did = order.tie, order.did
        chunks = list(reversed(range(NB)))

        wo2 = wo.reshape(hl * hd, d)
        wo_cross = cross(wo2)
        wo_same = same(wo2)
        wo_diag = same(wo_cross)

        xf = x.astype(f32)
        n1 = ((xf - mu1[:, None]) * rs1[:, None] * g1.astype(f32)).astype(bf)
        qkv = did(_dot(n1, wqkv).astype(bf))

        o_own, o_same, o_cross, o_diag = [], [], [], []
        npair = hl // 4
        prev = None
        for s in range(2):
            o, *prev = _attn_fwd(tie(qkv), hd, s * npair, npair, prev)
            did(o)
            oc = cross(o)
            o_own.append(split(o))
            o_cross.append(split(oc))
            o_same.append(split(same(o)))
            o_diag.append(split(same(oc)))
        o_all, lse, qkv_t = prev

        dg = did(_dot_t(tie(dy), w2))

        x4, dy4 = split(x), split(dy)
        xh2, rs2, n2, others = [None] * NB, [None] * NB, [None] * NB, [None] * NB
        for k in chunks:
            xh2[k], rs2[k], own, n2[k] = _h1(
                ids, k, tie(x4), o_own, o_same, o_cross, o_diag, (wo2, wo_same, wo_cross, wo_diag), g2[None]
            )
            did(own)
            others[k] = same(own)

        sums, n2f = [None] * NB, [None] * NB

        def place_n2(k):
            n2f[k] = did(_place(ids, tie(n2[k]), others[k])).reshape(b, d)

        def mlp(k, prev):
            res = _mlp(ids, tie(n2f[k]), w1, dg, k, prev)
            did(res[1])
            return res

        def partial_other(v, w):
            p = did(_dot_t(tie(v), w).astype(bf))
            return same(p)

        def partial_own(v, w, recv):
            s_own = did((_dot_t(tie(v), w) + recv.astype(f32)).astype(bf))
            return s_own, cross(s_own)

        def grad(u, v, add=None, keep=False):
            p = _dot(u.T, tie(v))
            p = p if add is None else p + add
            return did(p if keep else p.astype(bf))

        dh, dhb = [None] * NB, [None] * NB

        def norm2(k):
            dh[k], own, dhb[k] = _lnb(
                _lnb2_kernel, ids, k, (tie(sums[k][0]), sums[k][1], xh2[k], rs2[k], dy4, g2[None]),
                ("flat", "flat", "flat", "flat", "own", "gain"),
                (sds((r, d), f32), sds((r, d), bf), sds((2, r, d), bf)), ("flat", "flat", "pair"),
            )
            did(own)
            return same(own)

        def attention(k, other, acc, full):
            dhb[k] = did(_place(ids, tie(dhb[k]), other)).reshape(b, d)
            do = did(_dot_t(tie(dhb[k]), wo2).astype(bf))
            res = _attn_bwd(ids, qkv, qkv_t, o_all, do, lse, acc, full, k, b, hd)
            did(res[0])
            return res

        def norm1(k, pair, dx):
            args = (tie(pair[0]), pair[1], x4, mu4, rs4, dh[k], g1[None]) + (() if dx is None else (dx,))
            own, dx = _lnb(
                _lnb1_kernel, ids, k, args, ("flat", "flat", "own", "stat", "stat", "flat", "gain", "any")[: len(args)],
                (sds((r, d), bf), sds((NB, 2, r, d), bf)), ("flat", "own"),
                None if dx is None else {8: 1},
            )
            did(own)
            return same(own), dx

        place_n2(1)
        *gd, da_own, da_other = mlp(1, ())
        recv = partial_other(da_other, w1)
        place_n2(0)
        sums[1] = partial_own(da_own, w1, recv)
        gl, da, da_own, da_other = mlp(0, gd)
        recv = partial_other(da_other, w1)
        dw2 = grad(gl, dy)
        other = norm2(1)
        sums[0] = partial_own(da_own, w1, recv)

        mu4, rs4 = mu1.reshape(NB, 2, 1, r), rs1.reshape(NB, 2, 1, r)
        o3 = o_all.reshape(NB, b, -1)

        own1, oth1, full, acc = attention(1, other, None, None)
        recv = partial_other(oth1, wqkv)
        other = norm2(0)
        pair1 = partial_own(own1, wqkv, recv)
        own0, oth0, full = attention(0, other, acc, full)
        recv = partial_other(oth0, wqkv)
        dwo = grad(o3[1], dhb[1], keep=True)
        pair0 = partial_own(own0, wqkv, recv)
        dwo = grad(o3[0], dhb[0], dwo).reshape(hl, hd, d)
        dw1 = grad(jnp.concatenate(n2f, 0), da)
        other1, dx = norm1(1, pair1, None)
        dwqkv = grad(n1, full)
        other0, dx = norm1(0, pair0, dx)
        dx = _place4(ids, dx, other1, 1)
        dx = _place4(ids, dx, other0, 0)
        return dx.reshape(t, d), dwqkv, dwo, dw1, dw2

    return jax.shard_map(
        body, mesh=mesh,
        in_specs=(P("dp", None), P("dp"), P("dp"), P(None), P(None), P("dp", None),
                  P(None, "tp"), P("tp", None, None), P(None, "tp"), P("tp", None)),
        out_specs=(P("dp", None), P("dp", "tp"), P(("dp", "tp"), None, None), P("dp", "tp"), P(("dp", "tp"), None)),
        check_vma=False)
```

```python
import functools

import jax
import jax.numpy as jnp
from jax import lax
from jax.experimental import pallas as pl
from jax.experimental.pallas import tpu as pltpu
from jax.sharding import PartitionSpec as P


EPS = 1.0 / 100000
LOG2E = 1.4426950408889634
f32 = jnp.float32
bf = jnp.bfloat16
NB = 2
BQ = 256
TILE = 256
MB = 2**20
SAME = [(0, 1), (1, 0), (2, 3), (3, 2)]
MESH = pl.DeviceIdType.MESH
CROSS = [(0, 2), (2, 0), (1, 3), (3, 1)]


def _dot(a, b):
    return jnp.dot(a, b, preferred_element_type=f32)


def _dot_t(a, b):
    return lax.dot_general(a, b, (((1,), (1,)), ((), ())), preferred_element_type=f32)


def _causal(n):
    return lax.broadcasted_iota(jnp.int32, (n, n), 0) >= lax.broadcasted_iota(jnp.int32, (n, n), 1)


def _params(mb=60):
    return pltpu.CompilerParams(vmem_limit_bytes=mb * MB)


def _cost(flops, nbytes):
    return pl.CostEstimate(flops=int(flops), bytes_accessed=int(nbytes), transcendentals=0)


def _fwd_kernel(*refs, hd, r0, r1, first):
    if first:
        qkv_ref, o_ref, lse_ref, tr_ref = refs
        for i in range(r0 // BQ):
            rows = slice(i * BQ, (i + 1) * BQ)
            tr_ref[0, :, rows] = qkv_ref[rows, :].T
    else:
        qkv_ref, tr_ref, o_ref, lse_ref = refs
    c = LOG2E * hd**-0.5
    for i in range(r0 // BQ, r1 // BQ):
        w = (i + 1) * BQ
        rows = slice(i * BQ, w)
        loc = slice(i * BQ - r0, w - r0)
        blk = qkv_ref[rows, :]
        if first:
            tr_ref[0, :, rows] = blk.T
        scores = []
        for h in range(2):
            q = blk[:, 3 * hd * h : 3 * hd * h + hd]
            kt = slice(3 * hd * h + hd, 3 * hd * h + 2 * hd)
            s = _dot(q, tr_ref[0, kt, :w])
            d = jnp.where(_causal(BQ), s[:, w - BQ :], -jnp.inf)
            scores.append(jnp.concatenate([s[:, : w - BQ], d], 1) if i else d)
        cols, ps = [], []
        for s in scores:
            m = jnp.max(s, axis=1, keepdims=True)
            p = jnp.exp2((s - m) * c)
            l = jnp.sum(p, axis=1, keepdims=True)
            cols += [m * c + jnp.log2(l), 1.0 / l]
            ps.append(p.astype(bf))
        st = jnp.concatenate(cols, 1).T
        outs = []
        for h in range(2):
            vt = slice(3 * hd * h + 2 * hd, 3 * hd * h + 3 * hd)
            outs.append((_dot_t(tr_ref[0, vt, :w], ps[h]) * st[2 * h + 1 : 2 * h + 2]).astype(bf))
            lse_ref[0, h : h + 1, loc] = st[2 * h : 2 * h + 1]
        o_ref[loc, :] = jnp.concatenate(outs, 0).T


def _attn_fwd(qkv, hd, chunk, b, tr):
    t, w = qkv.shape
    npair = w // (6 * hd)
    r0, r1 = chunk * b, (chunk + 1) * b
    first = tr is None
    trans = pl.BlockSpec((1, 6 * hd, r1), lambda p: (p, 0, 0))
    res = pl.pallas_call(
        functools.partial(_fwd_kernel, hd=hd, r0=r0, r1=r1, first=first),
        grid=(npair,),
        in_specs=[pl.BlockSpec((r1, 6 * hd), lambda p: (0, p))] + ([] if first else [trans]),
        out_specs=[pl.BlockSpec((b, 2 * hd), lambda p: (0, p)), pl.BlockSpec((1, 2, b), lambda p: (p, 0, 0))]
        + ([trans] if first else []),
        out_shape=[jax.ShapeDtypeStruct((b, npair * 2 * hd), bf), jax.ShapeDtypeStruct((npair, 2, b), f32)]
        + ([jax.ShapeDtypeStruct((npair, 6 * hd, t), bf)] if first else []),
        compiler_params=_params(),
        cost_estimate=_cost(npair * 2 * b * (r0 + r1) * 1200, npair * 2 * t * hd * 16),
    )(qkv, *([] if first else [tr]))
    return (*res, tr)[:3]


def _bwd_kernel(*refs, hd, r0, r1, has_in, has_out):
    ids, qkv_ref, tr_ref, o_ref, do_ref, lse_ref = refs[:6]
    refs = refs[6:]
    acc_in = None
    if has_in:
        acc_in, _ = refs[:2]
        refs = refs[2:]
    pair_ref, full_ref = refs[:2]
    refs = refs[2:]
    acc_out = None
    if has_out:
        acc_out = refs[0]
        refs = refs[1:]
    (g_t,) = refs
    sc = hd**-0.5
    c = LOG2E * sc
    if has_in:
        g_t[...] = acc_in[0]
    for i in reversed(range(r0 // BQ, r1 // BQ)):
        w = (i + 1) * BQ
        rows = slice(i * BQ, w)
        loc = slice(i * BQ - r0, w - r0)
        blk = qkv_ref[loc, 0 : 4 * hd]
        do2 = do_ref[loc, :]
        do_t = do2.T
        lse = lse_ref[0, :, loc].T
        prod = do2.astype(f32) * o_ref[loc, :].astype(f32)
        sd = []
        for h in range(2):
            b = 3 * hd * h
            s = _dot(blk[:, b : b + hd], tr_ref[0, b + hd : b + 2 * hd, :w])
            dp = _dot(do2[:, h * hd : (h + 1) * hd], tr_ref[0, b + 2 * hd : b + 3 * hd, :w])
            sd.append((s, dp))
        ew = []
        for h in range(2):
            s, dp = sd[h]
            p = jnp.exp2(s * c - lse[:, h : h + 1])
            d = jnp.where(_causal(BQ), p[:, w - BQ :], 0.0)
            p = jnp.concatenate([p[:, : w - BQ], d], 1) if i else d
            delta = jnp.sum(prod[:, h * hd : (h + 1) * hd], axis=1, keepdims=True)
            ew.append((p.astype(bf), (p * (dp - delta)).astype(bf)))
        outs = []
        for h in range(2):
            p, ds = ew[h]
            b = 3 * hd * h
            dv = _dot(do_t[h * hd : (h + 1) * hd], p)
            dk = _dot(tr_ref[0, b : b + hd, rows], ds)
            dq = _dot_t(tr_ref[0, b + hd : b + 2 * hd, :w], ds)
            kr = slice(2 * hd * h, 2 * hd * h + hd)
            vr = slice(2 * hd * h + hd, 2 * hd * h + 2 * hd)
            if w == r1 and not has_in:
                g_t[kr, :] = dk
                g_t[vr, :] = dv
            else:
                g_t[kr, :w] += dk
                g_t[vr, :w] += dv
            outs += [(dq * sc).astype(bf), (g_t[kr, rows] * sc).astype(bf), g_t[vr, rows].astype(bf)]
        full_ref[loc, :] = jnp.concatenate(outs, 0).T
    half = (r1 - r0) // 2
    pair_ref[0, 0] = full_ref[pl.ds(pl.multiple_of(ids[0] * half, half), half), :]
    pair_ref[0, 1] = full_ref[pl.ds(pl.multiple_of((1 - ids[0]) * half, half), half), :]
    if has_out:
        acc_out[0] = g_t[:, :r0]


def _attn_bwd(ids, qkv, tr, o, do, lse, acc, full, chunk, b, hd):
    t, w = qkv.shape
    npair = w // (6 * hd)
    r0, r1 = chunk * b, (chunk + 1) * b
    has_in, has_out = acc is not None, r0 > 0
    in_specs = [
        pl.BlockSpec((b, 6 * hd), lambda p, s: (chunk, p)),
        pl.BlockSpec((1, 6 * hd, r1), lambda p, s: (p, 0, 0)),
        pl.BlockSpec((b, 2 * hd), lambda p, s: (0, p)),
        pl.BlockSpec((b, 2 * hd), lambda p, s: (0, p)),
        pl.BlockSpec((1, 2, b), lambda p, s: (p, 0, 0)),
    ]
    args = [qkv, tr, o, do, lse]
    alias = {}
    if has_in:
        in_specs += [pl.BlockSpec((1, 4 * hd, r1), lambda p, s: (p, 0, 0)), pl.BlockSpec(memory_space=pl.ANY)]
        args += [acc, full]
        alias = {7: 1}
    out_specs = [pl.BlockSpec((1, 2, b // 2, 6 * hd), lambda p, s: (0, 0, 0, p)), pl.BlockSpec((b, 6 * hd), lambda p, s: (chunk, p))]
    out_shape = [jax.ShapeDtypeStruct((1, 2, b // 2, w), bf), jax.ShapeDtypeStruct((t, w), bf)]
    if has_out:
        out_specs.append(pl.BlockSpec((1, 4 * hd, r0), lambda p, s: (p, 0, 0)))
        out_shape.append(jax.ShapeDtypeStruct((npair, 4 * hd, r0), f32))
    work = npair * 2 * b * (r0 + r1)
    return pl.pallas_call(
        functools.partial(_bwd_kernel, hd=hd, r0=r0, r1=r1, has_in=has_in, has_out=has_out),
        grid_spec=pltpu.PrefetchScalarGridSpec(
            num_scalar_prefetch=1,
            grid=(npair,),
            in_specs=in_specs,
            out_specs=out_specs,
            scratch_shapes=[pltpu.VMEM((4 * hd, r1), f32)],
        ),
        out_shape=out_shape,
        input_output_aliases=alias,
        compiler_params=_params(),
        cost_estimate=_cost(work * 1500, 3 * t * w),
    )(ids, *args)


def _h1_kernel(ids, x_ref, oa, ob, oc, od, wa, wb, wc, wd, g_ref, xh_ref, rs_ref, own_ref, acc):
    def run(first, second):
        acc[...] = sum(_dot(o[0], w[...]) for o, w in first + second)

    near, far = [(oa, wa), (ob, wb)], [(oc, wc), (od, wd)]

    @pl.when(ids[1] == 0)
    def _():
        run(near, far)

    @pl.when(ids[1] != 0)
    def _():
        run(far, near)

    h1 = x_ref[0, 0].astype(f32) + acc[...]
    xc = h1 - jnp.mean(h1, axis=1, keepdims=True)
    rs = lax.rsqrt(jnp.mean(xc * xc, axis=1, keepdims=True) + EPS)
    xh = xc * rs
    n2 = (xh * g_ref[...].astype(f32)).astype(bf)
    xh_ref[...] = xh
    rs_ref[...] = jnp.broadcast_to(rs, (rs.shape[0], 128))
    own_ref[...] = n2


def _h1(ids, chunk, x4, os, ws, g2):
    _, _, r, d = x4.shape
    k = os[0].shape[-1]
    flat = lambda n: pl.BlockSpec((TILE, n), lambda i, s: (i, 0))
    const = lambda shape: pl.BlockSpec(shape, lambda i, s: (0, 0), pipeline_mode=pl.Buffered(1))
    return pl.pallas_call(
        _h1_kernel,
        grid_spec=pltpu.PrefetchScalarGridSpec(
            num_scalar_prefetch=1,
            grid=(r // TILE,),
            in_specs=[pl.BlockSpec((1, 1, TILE, d), lambda i, s: (chunk, s[0], i, 0))]
            + [pl.BlockSpec((1, TILE, k), lambda i, s: (s[0], i, 0))] * 4
            + [const((k, d))] * 4
            + [const((1, d))],
            out_specs=[flat(d), flat(128), flat(d)],
            scratch_shapes=[pltpu.VMEM((TILE, d), f32)],
        ),
        out_shape=[
            jax.ShapeDtypeStruct((r, d), f32),
            jax.ShapeDtypeStruct((r, 128), f32),
            jax.ShapeDtypeStruct((r, d), bf),
        ],
        compiler_params=_params(),
        cost_estimate=_cost(8 * r * d * k, 20 * MB),
    )(ids, x4, *os, *ws, g2)


GC0 = 0.7978845608028654
GC1 = 0.044715


def _mlp_kernel(ids, own_n, other_n, w_ref, dg_ref, *refs):
    gl_ref, da_ref, n_ref = refs[-3:]
    sub = own_n.shape[0]
    core = ids[0]
    for half, at, src in ((0, core, own_n), (1, 1 - core, other_n)):
        rows = pl.ds(pl.multiple_of(at * sub, sub), sub)
        a = _dot(src[...], w_ref[...])
        a2 = a * a
        h = 0.5 + 0.5 * jnp.tanh(a * (GC0 + GC0 * GC1 * a2))
        gl_ref[rows, :] = (a * h).astype(bf)
        slope = h + a * (h * (1.0 - h)) * (2.0 * GC0 + 6.0 * GC0 * GC1 * a2)
        da_ref[0, half] = (dg_ref[rows, :] * slope).astype(bf)

    @pl.when(pl.program_id(0) == 0)
    def _():
        n_ref[0, 0] = own_n[...]
        n_ref[0, 1] = other_n[...]


def _mlp(ids, own, other, w1, dg, chunk, prev, bn=512):
    r, d = own.shape
    t, f = dg.shape
    spec = pl.BlockSpec((2 * r, bn), lambda j, s: (chunk, j))
    pair = lambda k, f: pl.BlockSpec((1, 2, r, k), f)
    rows = pl.BlockSpec((r, d), lambda j, s: (0, 0), pipeline_mode=pl.Buffered(1))
    return pl.pallas_call(
        _mlp_kernel,
        grid_spec=pltpu.PrefetchScalarGridSpec(
            num_scalar_prefetch=1,
            grid=(f // bn,),
            in_specs=[rows, rows, pl.BlockSpec((d, bn), lambda j, s: (0, j)), spec]
            + [pl.BlockSpec(memory_space=pl.ANY)] * len(prev),
            out_specs=[spec, pair(bn, lambda j, s: (chunk, 0, 0, j)), pair(d, lambda j, s: (chunk, 0, 0, 0))],
        ),
        out_shape=[
            jax.ShapeDtypeStruct((t, f), bf),
            jax.ShapeDtypeStruct((NB, 2, r, f), bf),
            jax.ShapeDtypeStruct((NB, 2, r, d), bf),
        ],
        input_output_aliases={5: 0, 6: 1, 7: 2} if prev else {},
        compiler_params=_params(),
        cost_estimate=_cost(4 * r * d * f * 1.3, 4 * r * f * 8),
    )(ids, own, other, w1, dg, *prev)


def _partial_kernel(v_ref, w_ref, out_ref, sent, got, send_sem, recv_sem, *, nt):
    j = pl.program_id(0)
    me = lax.axis_index("tp")
    peer = {"tp": me + 1 - 2 * lax.rem(me, 2)}

    def copy(i):
        return pltpu.make_async_remote_copy(
            src_ref=sent.at[i], dst_ref=got.at[i], send_sem=send_sem.at[i], recv_sem=recv_sem.at[i],
            device_id=peer, device_id_type=MESH,
        )

    @pl.when(j == 0)
    def _():
        barrier = pltpu.get_barrier_semaphore()
        pl.semaphore_signal(barrier, inc=1, device_id=peer, device_id_type=MESH)
        pl.semaphore_wait(barrier, 1)

    @pl.when((j >= 1) & (j <= nt))
    def _():
        copy(j - 1).start()

    @pl.when(j < nt)
    def _():
        sent[j] = _dot_t(v_ref[0, 0], w_ref[...]).astype(bf)

    @pl.when(j >= nt)
    def _():
        p = _dot_t(v_ref[0, 0], w_ref[...])
        copy(j - nt).wait_recv()
        out_ref[...] = (p + got[j - nt].astype(f32)).astype(bf)

    @pl.when(j == 2 * nt - 1)
    def _():
        for i in range(nt):
            copy(i).wait_send()


def _partial(v4, chunk, w, cid, nt):
    _, _, r, k = v4.shape
    n = w.shape[0]
    bn = n // nt
    return pl.pallas_call(
        functools.partial(_partial_kernel, nt=nt),
        grid=(2 * nt,),
        in_specs=[
            pl.BlockSpec((1, 1, r, k), lambda j: (chunk, 1 - j // nt, 0, 0)),
            pl.BlockSpec((bn, k), lambda j: (lax.rem(j, nt), 0)),
        ],
        out_specs=pl.BlockSpec((r, bn), lambda j: (0, jnp.maximum(j - nt, 0))),
        out_shape=jax.ShapeDtypeStruct((r, n), bf),
        scratch_shapes=[
            pltpu.VMEM((nt, r, bn), bf),
            pltpu.VMEM((nt, r, bn), bf),
            pltpu.SemaphoreType.DMA((nt,)),
            pltpu.SemaphoreType.DMA((nt,)),
        ],
        compiler_params=pltpu.CompilerParams(vmem_limit_bytes=60 * MB, collective_id=cid, has_side_effects=True),
        cost_estimate=_cost(4 * r * k * n, 6 * r * k + 2 * n * k),
    )(v4, w)


def _place_kernel(ids, v_ref, _, buf_ref):
    buf_ref[0] = v_ref[...]


def _place(ids, buf, v):
    r, d = v.shape
    return pl.pallas_call(
        _place_kernel,
        grid_spec=pltpu.PrefetchScalarGridSpec(
            num_scalar_prefetch=1,
            grid=(r // TILE,),
            in_specs=[pl.BlockSpec((TILE, d), lambda i, s: (i, 0)), pl.BlockSpec(memory_space=pl.ANY)],
            out_specs=pl.BlockSpec((1, TILE, d), lambda i, s: (1 - s[0], i, 0)),
        ),
        out_shape=jax.ShapeDtypeStruct(buf.shape, buf.dtype),
        input_output_aliases={2: 0},
        compiler_params=_params(32),
        cost_estimate=_cost(r * d * 1000, 2 * r * d * 2),
    )(ids, v, buf)


def _place4_kernel(ids, v_ref, _, buf_ref):
    buf_ref[0, 0] = v_ref[...]


def _place4(ids, buf, v, chunk):
    r, d = v.shape
    return pl.pallas_call(
        _place4_kernel,
        grid_spec=pltpu.PrefetchScalarGridSpec(
            num_scalar_prefetch=1,
            grid=(r // TILE,),
            in_specs=[pl.BlockSpec((TILE, d), lambda i, s: (i, 0)), pl.BlockSpec(memory_space=pl.ANY)],
            out_specs=pl.BlockSpec((1, 1, TILE, d), lambda i, s: (chunk, 1 - s[0], i, 0)),
        ),
        out_shape=jax.ShapeDtypeStruct(buf.shape, buf.dtype),
        input_output_aliases={2: 0},
        compiler_params=_params(32),
        cost_estimate=_cost(r * d * 1000, 2 * r * d * 2),
    )(ids, v, buf)


def _lnb2_kernel(ids, sa, sb, xh_ref, rs_ref, dy_ref, g_ref, dh_ref, own_ref, full_ref):
    u = (sa[...].astype(f32) + sb[...].astype(f32)) * g_ref[...].astype(f32)
    xh = xh_ref[...]
    v = u - jnp.mean(u, axis=1, keepdims=True) - xh * jnp.mean(u * xh, axis=1, keepdims=True)
    dh = dy_ref[0, 0].astype(f32) + rs_ref[:, :1] * v
    dhb = dh.astype(bf)
    dh_ref[...] = dh
    own_ref[...] = dhb
    full_ref[0] = dhb


def _lnb1_kernel(ids, sa, sb, x_ref, mu_ref, rs_ref, dh_ref, g_ref, *outs):
    u = (sa[...].astype(f32) + sb[...].astype(f32)) * g_ref[...].astype(f32)
    rs = rs_ref[0, 0].T
    xh = (x_ref[0, 0].astype(f32) - mu_ref[0, 0].T) * rs
    v = u - jnp.mean(u, axis=1, keepdims=True) - xh * jnp.mean(u * xh, axis=1, keepdims=True)
    dx = (dh_ref[...] + rs * v).astype(bf)
    outs[-2][...] = dx
    outs[-1][0, 0] = dx


def _lnb(kernel, ids, chunk, args, kinds, outs, out_kinds, alias=None, tile=128):
    r = args[0].shape[0]
    specs = {
        "flat": lambda k: pl.BlockSpec((tile, k), lambda i, s: (i, 0)),
        "own": lambda k: pl.BlockSpec((1, 1, tile, k), lambda i, s: (chunk, s[0], i, 0)),
        "stat": lambda k: pl.BlockSpec((1, 1, 1, tile), lambda i, s: (chunk, s[0], 0, i)),
        "gain": lambda k: pl.BlockSpec((1, k), lambda i, s: (0, 0)),
        "pair": lambda k: pl.BlockSpec((1, tile, k), lambda i, s: (s[0], i, 0)),
        "any": lambda k: pl.BlockSpec(memory_space=pl.ANY),
    }
    return pl.pallas_call(
        kernel,
        grid_spec=pltpu.PrefetchScalarGridSpec(
            num_scalar_prefetch=1,
            grid=(r // tile,),
            in_specs=[specs[k](a.shape[-1]) for k, a in zip(kinds, args)],
            out_specs=[specs[k](o.shape[-1]) for k, o in zip(out_kinds, outs)],
        ),
        out_shape=outs,
        input_output_aliases=alias or {},
        compiler_params=_params(32),
        cost_estimate=_cost(r * 2048 * 6000, r * 2048 * 16),
    )(ids, *args)


class _Chain:
    def __init__(self):
        self.last = None

    def tie(self, *args):
        if self.last is not None:
            *args, _ = lax.optimization_barrier((*args, self.last))
        return args if len(args) > 1 else args[0]

    def did(self, v):
        self.last = v
        return v


def solution(mesh):
    def body(x, mu1, rs1, g1, g2, dy, wqkv, wo, w1, w2):
        hl, hd, d = wo.shape
        t = x.shape[0]
        b = t // NB
        r = b // 2
        me = lax.axis_index("tp")
        core, chip = me % 2, me // 2
        ids = jnp.stack([core, chip]).astype(jnp.int32)

        def same(v):
            return lax.ppermute(v, "tp", SAME)

        def cross(v):
            return lax.ppermute(v, "tp", CROSS)

        split = lambda v: v.reshape(NB, 2, r, v.shape[-1])
        sds = jax.ShapeDtypeStruct
        order = _Chain()
        tie, did = order.tie, order.did
        chunks = list(reversed(range(NB)))

        wo2 = wo.reshape(hl * hd, d)
        wo_cross = cross(wo2)
        wo_same = same(wo2)
        wo_diag = same(wo_cross)

        xf = x.astype(f32)
        n1 = ((xf - mu1[:, None]) * rs1[:, None] * g1.astype(f32)).astype(bf)
        qkv = did(_dot(n1, wqkv).astype(bf))

        pair_rows = lambda v: v.reshape(2, r, v.shape[-1])
        o, lse, os = [None] * NB, [None] * NB, [None] * NB
        qkv_t = None
        for k in chunks:
            o[k], lse[k], qkv_t = _attn_fwd(tie(qkv), hd, k, b, qkv_t)
            did(o[k])
            o_cross = cross(o[k])
            o_same, o_diag = same(o[k]), same(o_cross)
            os[k] = [pair_rows(v) for v in (o[k], o_same, o_cross, o_diag)]

        dg = did(_dot_t(tie(dy), w2))

        x4, dy4 = split(x), split(dy)
        xh2, rs2, n2, others = [None] * NB, [None] * NB, [None] * NB, [None] * NB
        for k in chunks:
            xh2[k], rs2[k], n2[k] = _h1(
                ids, k, tie(x4), os[k], (wo2, wo_same, wo_cross, wo_diag), g2[None]
            )
            did(n2[k])
            others[k] = same(n2[k])

        sums = [None] * NB

        def mlp(k, prev):
            res = _mlp(ids, tie(n2[k]), others[k], w1, dg, k, prev)
            did(res[1])
            return res

        def partial(v4, k, w, cid):
            s_own = did(_partial(tie(v4), k, w, cid, 2))
            return s_own, cross(s_own)

        def grad(u, v, add=None, keep=False):
            p = _dot(u.T, tie(v))
            p = p if add is None else p + add
            return did(p if keep else p.astype(bf))

        dh, dhb = [None] * NB, [None] * NB

        def norm2(k):
            dh[k], own, dhb[k] = _lnb(
                _lnb2_kernel, ids, k, (tie(sums[k][0]), sums[k][1], xh2[k], rs2[k], dy4, g2[None]),
                ("flat", "flat", "flat", "flat", "own", "gain"),
                (pltpu.HBM((r, d), f32), sds((r, d), bf), sds((2, r, d), bf)), ("flat", "flat", "pair"),
            )
            did(own)
            return same(own)

        def attention(k, other, acc, full):
            dhb[k] = did(_place(ids, tie(dhb[k]), other)).reshape(b, d)
            do = did(_dot_t(tie(dhb[k]), wo2).astype(bf))
            res = _attn_bwd(ids, qkv, qkv_t, o[k], do, lse[k], acc, full, k, b, hd)
            did(res[0])
            return res

        def norm1(k, pair, dx):
            args = (tie(pair[0]), pair[1], x4, mu4, rs4, dh[k], g1[None]) + (() if dx is None else (dx,))
            own, dx = _lnb(
                _lnb1_kernel, ids, k, args, ("flat", "flat", "own", "stat", "stat", "flat", "gain", "any")[: len(args)],
                (sds((r, d), bf), sds((NB, 2, r, d), bf)), ("flat", "own"),
                None if dx is None else {8: 1},
            )
            did(own)
            return same(own), dx

        gd = mlp(1, ())
        sums[1] = partial(gd[1], 1, w1, 1)
        gl, da, n2_all = mlp(0, gd)
        dw2 = grad(gl, dy)
        other = norm2(1)
        sums[0] = partial(da, 0, w1, 2)

        mu4, rs4 = mu1.reshape(NB, 2, 1, r), rs1.reshape(NB, 2, 1, r)

        pair, full, acc = attention(1, other, None, None)
        pair1 = partial(pair, 0, wqkv, 3)
        other = norm2(0)
        dwo = grad(o[1], dhb[1], keep=True)
        pair, full = attention(0, other, acc, full)
        pair0 = partial(pair, 0, wqkv, 4)
        dwo = grad(o[0], dhb[0], dwo).reshape(hl, hd, d)
        dw1 = grad(n2_all.reshape(t, d), da.reshape(t, -1))
        other1, dx = norm1(1, pair1, None)
        dwqkv = grad(n1, full)
        other0, dx = norm1(0, pair0, dx)
        dx = _place4(ids, dx, other1, 1)
        dx = _place4(ids, dx, other0, 0)
        return dx.reshape(t, d), dwqkv, dwo, dw1, dw2

    return jax.shard_map(
        body, mesh=mesh,
        in_specs=(P("dp", None), P("dp"), P("dp"), P(None), P(None), P("dp", None),
                  P(None, "tp"), P("tp", None, None), P(None, "tp"), P("tp", None)),
        out_specs=(P("dp", None), P("dp", "tp"), P(("dp", "tp"), None, None), P("dp", "tp"), P(("dp", "tp"), None)),
        check_vma=False)
```

```python
import functools

import jax
import jax.numpy as jnp
from jax import lax
from jax.experimental import pallas as pl
from jax.experimental.pallas import tpu as pltpu
from jax.sharding import PartitionSpec as P


EPS = 1.0 / 100000
LOG2E = 1.4426950408889634
f32 = jnp.float32
bf = jnp.bfloat16
NB = 2
BQ = 256
TILE = 256
MB = 2**20
SAME = [(0, 1), (1, 0), (2, 3), (3, 2)]
MESH = pl.DeviceIdType.MESH
CROSS = [(0, 2), (2, 0), (1, 3), (3, 1)]


def _dot(a, b):
    return jnp.dot(a, b, preferred_element_type=f32)


def _dot_t(a, b):
    return lax.dot_general(a, b, (((1,), (1,)), ((), ())), preferred_element_type=f32)


def _causal(n):
    return lax.broadcasted_iota(jnp.int32, (n, n), 0) >= lax.broadcasted_iota(jnp.int32, (n, n), 1)


def _params(mb=60):
    return pltpu.CompilerParams(vmem_limit_bytes=mb * MB)


def _cost(flops, nbytes):
    return pl.CostEstimate(flops=int(flops), bytes_accessed=int(nbytes), transcendentals=0)


def _fwd_kernel(*refs, hd, r0, r1, first):
    if first:
        qkv_ref, o_ref, lse_ref, tr_ref = refs
        for i in range(r0 // BQ):
            rows = slice(i * BQ, (i + 1) * BQ)
            tr_ref[0, :, rows] = qkv_ref[rows, :].T
    else:
        qkv_ref, tr_ref, o_ref, lse_ref = refs
    c = LOG2E * hd**-0.5
    for i in range(r0 // BQ, r1 // BQ):
        w = (i + 1) * BQ
        rows = slice(i * BQ, w)
        loc = slice(i * BQ - r0, w - r0)
        blk = qkv_ref[rows, :]
        if first:
            tr_ref[0, :, rows] = blk.T
        scores = []
        for h in range(2):
            q = blk[:, 3 * hd * h : 3 * hd * h + hd]
            kt = slice(3 * hd * h + hd, 3 * hd * h + 2 * hd)
            s = _dot(q, tr_ref[0, kt, :w])
            d = jnp.where(_causal(BQ), s[:, w - BQ :], -jnp.inf)
            scores.append(jnp.concatenate([s[:, : w - BQ], d], 1) if i else d)
        cols, ps = [], []
        for s in scores:
            m = jnp.max(s, axis=1, keepdims=True)
            p = jnp.exp2((s - m) * c)
            l = jnp.sum(p, axis=1, keepdims=True)
            cols += [m * c + jnp.log2(l), 1.0 / l]
            ps.append(p.astype(bf))
        st = jnp.concatenate(cols, 1).T
        outs = []
        for h in range(2):
            vt = slice(3 * hd * h + 2 * hd, 3 * hd * h + 3 * hd)
            outs.append((_dot_t(tr_ref[0, vt, :w], ps[h]) * st[2 * h + 1 : 2 * h + 2]).astype(bf))
            lse_ref[0, h : h + 1, loc] = st[2 * h : 2 * h + 1]
        o_ref[loc, :] = jnp.concatenate(outs, 0).T


def _attn_fwd(qkv, hd, chunk, b, tr):
    t, w = qkv.shape
    npair = w // (6 * hd)
    r0, r1 = chunk * b, (chunk + 1) * b
    first = tr is None
    trans = pl.BlockSpec((1, 6 * hd, r1), lambda p: (p, 0, 0))
    res = pl.pallas_call(
        functools.partial(_fwd_kernel, hd=hd, r0=r0, r1=r1, first=first),
        grid=(npair,),
        in_specs=[pl.BlockSpec((r1, 6 * hd), lambda p: (0, p))] + ([] if first else [trans]),
        out_specs=[pl.BlockSpec((b, 2 * hd), lambda p: (0, p)), pl.BlockSpec((1, 2, b), lambda p: (p, 0, 0))]
        + ([trans] if first else []),
        out_shape=[jax.ShapeDtypeStruct((b, npair * 2 * hd), bf), jax.ShapeDtypeStruct((npair, 2, b), f32)]
        + ([jax.ShapeDtypeStruct((npair, 6 * hd, t), bf)] if first else []),
        compiler_params=_params(36),
        cost_estimate=_cost(npair * 2 * b * (r0 + r1) * 1200, npair * 2 * t * hd * 16),
    )(qkv, *([] if first else [tr]))
    return (*res, tr)[:3]


def _bwd_kernel(*refs, hd, r0, r1, has_in, has_out):
    ids, qkv_ref, tr_ref, o_ref, do_ref, lse_ref = refs[:6]
    refs = refs[6:]
    acc_in = None
    if has_in:
        acc_in, _ = refs[:2]
        refs = refs[2:]
    pair_ref, full_ref = refs[:2]
    refs = refs[2:]
    acc_out = None
    if has_out:
        acc_out = refs[0]
        refs = refs[1:]
    (g_t,) = refs
    sc = hd**-0.5
    c = LOG2E * sc
    if has_in:
        g_t[...] = acc_in[0]
    for i in reversed(range(r0 // BQ, r1 // BQ)):
        w = (i + 1) * BQ
        rows = slice(i * BQ, w)
        loc = slice(i * BQ - r0, w - r0)
        blk = qkv_ref[loc, 0 : 4 * hd]
        do2 = do_ref[loc, :]
        do_t = do2.T
        lse = lse_ref[0, :, loc].T
        prod = do2.astype(f32) * o_ref[loc, :].astype(f32)
        sd = []
        for h in range(2):
            b = 3 * hd * h
            s = _dot(blk[:, b : b + hd], tr_ref[0, b + hd : b + 2 * hd, :w])
            dp = _dot(do2[:, h * hd : (h + 1) * hd], tr_ref[0, b + 2 * hd : b + 3 * hd, :w])
            sd.append((s, dp))
        ew = []
        for h in range(2):
            s, dp = sd[h]
            p = jnp.exp2(s * c - lse[:, h : h + 1])
            d = jnp.where(_causal(BQ), p[:, w - BQ :], 0.0)
            p = jnp.concatenate([p[:, : w - BQ], d], 1) if i else d
            delta = jnp.sum(prod[:, h * hd : (h + 1) * hd], axis=1, keepdims=True)
            ew.append((p.astype(bf), (p * (dp - delta)).astype(bf)))
        outs = []
        for h in range(2):
            p, ds = ew[h]
            b = 3 * hd * h
            dv = _dot(do_t[h * hd : (h + 1) * hd], p)
            dk = _dot(tr_ref[0, b : b + hd, rows], ds)
            dq = _dot_t(tr_ref[0, b + hd : b + 2 * hd, :w], ds)
            kr = slice(2 * hd * h, 2 * hd * h + hd)
            vr = slice(2 * hd * h + hd, 2 * hd * h + 2 * hd)
            if w == r1 and not has_in:
                g_t[kr, :] = dk
                g_t[vr, :] = dv
            else:
                g_t[kr, :w] += dk
                g_t[vr, :w] += dv
            outs += [(dq * sc).astype(bf), (g_t[kr, rows] * sc).astype(bf), g_t[vr, rows].astype(bf)]
        full_ref[loc, :] = jnp.concatenate(outs, 0).T
    half = (r1 - r0) // 2
    pair_ref[0, 0] = full_ref[pl.ds(pl.multiple_of(ids[0] * half, half), half), :]
    pair_ref[0, 1] = full_ref[pl.ds(pl.multiple_of((1 - ids[0]) * half, half), half), :]
    if has_out:
        acc_out[0] = g_t[:, :r0]


def _attn_bwd(ids, qkv, tr, o, do, lse, acc, full, chunk, b, hd):
    t, w = qkv.shape
    npair = w // (6 * hd)
    r0, r1 = chunk * b, (chunk + 1) * b
    has_in, has_out = acc is not None, r0 > 0
    in_specs = [
        pl.BlockSpec((b, 6 * hd), lambda p, s: (chunk, p)),
        pl.BlockSpec((1, 6 * hd, r1), lambda p, s: (p, 0, 0)),
        pl.BlockSpec((b, 2 * hd), lambda p, s: (0, p)),
        pl.BlockSpec((b, 2 * hd), lambda p, s: (0, p)),
        pl.BlockSpec((1, 2, b), lambda p, s: (p, 0, 0)),
    ]
    args = [qkv, tr, o, do, lse]
    alias = {}
    if has_in:
        in_specs += [pl.BlockSpec((1, 4 * hd, r1), lambda p, s: (p, 0, 0)), pl.BlockSpec(memory_space=pl.ANY)]
        args += [acc, full]
        alias = {7: 1}
    out_specs = [pl.BlockSpec((1, 2, b // 2, 6 * hd), lambda p, s: (0, 0, 0, p)), pl.BlockSpec((b, 6 * hd), lambda p, s: (chunk, p))]
    out_shape = [pltpu.HBM((1, 2, b // 2, w), bf), pltpu.HBM((t, w), bf)]
    if has_out:
        out_specs.append(pl.BlockSpec((1, 4 * hd, r0), lambda p, s: (p, 0, 0)))
        out_shape.append(pltpu.HBM((npair, 4 * hd, r0), f32))
    work = npair * 2 * b * (r0 + r1)
    return pl.pallas_call(
        functools.partial(_bwd_kernel, hd=hd, r0=r0, r1=r1, has_in=has_in, has_out=has_out),
        grid_spec=pltpu.PrefetchScalarGridSpec(
            num_scalar_prefetch=1,
            grid=(npair,),
            in_specs=in_specs,
            out_specs=out_specs,
            scratch_shapes=[pltpu.VMEM((4 * hd, r1), f32)],
        ),
        out_shape=out_shape,
        input_output_aliases=alias,
        compiler_params=_params(44),
        cost_estimate=_cost(work * 1500, 3 * t * w),
    )(ids, *args)


def _h1_kernel(ids, x_ref, oa, ob, oc, od, wa, wb, wc, wd, g_ref, xh_ref, rs_ref, own_ref, acc):
    def run(first, second):
        acc[...] = sum(_dot(o[0], w[...]) for o, w in first + second)

    near, far = [(oa, wa), (ob, wb)], [(oc, wc), (od, wd)]

    @pl.when(ids[1] == 0)
    def _():
        run(near, far)

    @pl.when(ids[1] != 0)
    def _():
        run(far, near)

    h1 = x_ref[0, 0].astype(f32) + acc[...]
    xc = h1 - jnp.mean(h1, axis=1, keepdims=True)
    rs = lax.rsqrt(jnp.mean(xc * xc, axis=1, keepdims=True) + EPS)
    xh = xc * rs
    n2 = (xh * g_ref[...].astype(f32)).astype(bf)
    xh_ref[...] = xh
    rs_ref[...] = jnp.broadcast_to(rs, (rs.shape[0], 128))
    own_ref[...] = n2


def _h1(ids, chunk, x4, os, ws, g2):
    _, _, r, d = x4.shape
    k = os[0].shape[-1]
    flat = lambda n: pl.BlockSpec((TILE, n), lambda i, s: (i, 0))
    const = lambda shape: pl.BlockSpec(shape, lambda i, s: (0, 0), pipeline_mode=pl.Buffered(1))
    return pl.pallas_call(
        _h1_kernel,
        grid_spec=pltpu.PrefetchScalarGridSpec(
            num_scalar_prefetch=1,
            grid=(r // TILE,),
            in_specs=[pl.BlockSpec((1, 1, TILE, d), lambda i, s: (chunk, s[0], i, 0))]
            + [pl.BlockSpec((1, TILE, k), lambda i, s: (s[0], i, 0))] * 4
            + [const((k, d))] * 4
            + [const((1, d))],
            out_specs=[flat(d), flat(128), flat(d)],
            scratch_shapes=[pltpu.VMEM((TILE, d), f32)],
        ),
        out_shape=[
            jax.ShapeDtypeStruct((r, d), f32),
            jax.ShapeDtypeStruct((r, 128), f32),
            jax.ShapeDtypeStruct((r, d), bf),
        ],
        compiler_params=_params(36),
        cost_estimate=_cost(8 * r * d * k, 20 * MB),
    )(ids, x4, *os, *ws, g2)


GC0 = 0.7978845608028654
GC1 = 0.044715


def _mlp_kernel(ids, own_n, other_n, w_ref, dg_ref, *refs):
    gl_ref, da_ref, n_ref = refs[-3:]
    sub = own_n.shape[0]
    core = ids[0]
    for half, at, src in ((0, core, own_n), (1, 1 - core, other_n)):
        rows = pl.ds(pl.multiple_of(at * sub, sub), sub)
        a = _dot(src[...], w_ref[...])
        a2 = a * a
        h = 0.5 + 0.5 * jnp.tanh(a * (GC0 + GC0 * GC1 * a2))
        gl_ref[rows, :] = (a * h).astype(bf)
        slope = h + a * (h * (1.0 - h)) * (2.0 * GC0 + 6.0 * GC0 * GC1 * a2)
        da_ref[0, half] = (dg_ref[rows, :] * slope).astype(bf)

    @pl.when(pl.program_id(0) == 0)
    def _():
        n_ref[0, 0] = own_n[...]
        n_ref[0, 1] = other_n[...]


def _mlp(ids, own, other, w1, dg, chunk, prev, bn=512):
    r, d = own.shape
    t, f = dg.shape
    spec = pl.BlockSpec((2 * r, bn), lambda j, s: (chunk, j))
    pair = lambda k, f: pl.BlockSpec((1, 2, r, k), f)
    rows = pl.BlockSpec((r, d), lambda j, s: (0, 0), pipeline_mode=pl.Buffered(1))
    return pl.pallas_call(
        _mlp_kernel,
        grid_spec=pltpu.PrefetchScalarGridSpec(
            num_scalar_prefetch=1,
            grid=(f // bn,),
            in_specs=[rows, rows, pl.BlockSpec((d, bn), lambda j, s: (0, j)), spec]
            + [pl.BlockSpec(memory_space=pl.ANY)] * len(prev),
            out_specs=[spec, pair(bn, lambda j, s: (chunk, 0, 0, j)), pair(d, lambda j, s: (chunk, 0, 0, 0))],
        ),
        out_shape=[
            pltpu.HBM((t, f), bf),
            pltpu.HBM((NB, 2, r, f), bf),
            pltpu.HBM((NB, 2, r, d), bf),
        ],
        input_output_aliases={5: 0, 6: 1, 7: 2} if prev else {},
        compiler_params=_params(48),
        cost_estimate=_cost(4 * r * d * f * 1.3, 4 * r * f * 8),
    )(ids, own, other, w1, dg, *prev)


def _partial_kernel(v_ref, w_ref, out_ref, sent, got, send_sem, recv_sem, *, nt):
    j = pl.program_id(0)
    me = lax.axis_index("tp")
    peer = {"tp": me + 1 - 2 * lax.rem(me, 2)}

    def copy(i):
        return pltpu.make_async_remote_copy(
            src_ref=sent.at[i], dst_ref=got.at[i], send_sem=send_sem.at[i], recv_sem=recv_sem.at[i],
            device_id=peer, device_id_type=MESH,
        )

    @pl.when(j == 0)
    def _():
        barrier = pltpu.get_barrier_semaphore()
        pl.semaphore_signal(barrier, inc=1, device_id=peer, device_id_type=MESH)
        pl.semaphore_wait(barrier, 1)

    @pl.when((j >= 1) & (j <= nt))
    def _():
        copy(j - 1).start()

    @pl.when(j < nt)
    def _():
        sent[j] = _dot_t(v_ref[0, 0], w_ref[...]).astype(bf)

    @pl.when(j >= nt)
    def _():
        p = _dot_t(v_ref[0, 0], w_ref[...])
        copy(j - nt).wait_recv()
        out_ref[...] = (p + got[j - nt].astype(f32)).astype(bf)

    @pl.when(j == 2 * nt - 1)
    def _():
        for i in range(nt):
            copy(i).wait_send()


def _partial(v4, chunk, w, cid, nt):
    _, _, r, k = v4.shape
    n = w.shape[0]
    bn = n // nt
    return pl.pallas_call(
        functools.partial(_partial_kernel, nt=nt),
        grid=(2 * nt,),
        in_specs=[
            pl.BlockSpec((1, 1, r, k), lambda j: (chunk, 1 - j // nt, 0, 0)),
            pl.BlockSpec((bn, k), lambda j: (lax.rem(j, nt), 0)),
        ],
        out_specs=pl.BlockSpec((r, bn), lambda j: (0, jnp.maximum(j - nt, 0))),
        out_shape=jax.ShapeDtypeStruct((r, n), bf),
        scratch_shapes=[
            pltpu.VMEM((nt, r, bn), bf),
            pltpu.VMEM((nt, r, bn), bf),
            pltpu.SemaphoreType.DMA((nt,)),
            pltpu.SemaphoreType.DMA((nt,)),
        ],
        compiler_params=pltpu.CompilerParams(vmem_limit_bytes=44 * MB, collective_id=cid, has_side_effects=True),
        cost_estimate=_cost(4 * r * k * n, 6 * r * k + 2 * n * k),
    )(v4, w)


def _place_kernel(ids, v_ref, _, buf_ref):
    buf_ref[0] = v_ref[...]


def _place(ids, buf, v):
    r, d = v.shape
    return pl.pallas_call(
        _place_kernel,
        grid_spec=pltpu.PrefetchScalarGridSpec(
            num_scalar_prefetch=1,
            grid=(r // TILE,),
            in_specs=[pl.BlockSpec((TILE, d), lambda i, s: (i, 0)), pl.BlockSpec(memory_space=pl.ANY)],
            out_specs=pl.BlockSpec((1, TILE, d), lambda i, s: (1 - s[0], i, 0)),
        ),
        out_shape=jax.ShapeDtypeStruct(buf.shape, buf.dtype),
        input_output_aliases={2: 0},
        compiler_params=_params(32),
        cost_estimate=_cost(r * d * 1000, 2 * r * d * 2),
    )(ids, v, buf)


def _place4_kernel(ids, v_ref, _, buf_ref):
    buf_ref[0, 0] = v_ref[...]


def _place4(ids, buf, v, chunk):
    r, d = v.shape
    return pl.pallas_call(
        _place4_kernel,
        grid_spec=pltpu.PrefetchScalarGridSpec(
            num_scalar_prefetch=1,
            grid=(r // TILE,),
            in_specs=[pl.BlockSpec((TILE, d), lambda i, s: (i, 0)), pl.BlockSpec(memory_space=pl.ANY)],
            out_specs=pl.BlockSpec((1, 1, TILE, d), lambda i, s: (chunk, 1 - s[0], i, 0)),
        ),
        out_shape=jax.ShapeDtypeStruct(buf.shape, buf.dtype),
        input_output_aliases={2: 0},
        compiler_params=_params(32),
        cost_estimate=_cost(r * d * 1000, 2 * r * d * 2),
    )(ids, v, buf)


def _lnb2_kernel(ids, sa, sb, xh_ref, rs_ref, dy_ref, g_ref, dh_ref, own_ref, full_ref):
    u = (sa[...].astype(f32) + sb[...].astype(f32)) * g_ref[...].astype(f32)
    xh = xh_ref[...]
    v = u - jnp.mean(u, axis=1, keepdims=True) - xh * jnp.mean(u * xh, axis=1, keepdims=True)
    dh = dy_ref[0, 0].astype(f32) + rs_ref[:, :1] * v
    dhb = dh.astype(bf)
    dh_ref[...] = dh
    own_ref[...] = dhb
    full_ref[0] = dhb


def _lnb1_kernel(ids, sa, sb, x_ref, mu_ref, rs_ref, dh_ref, g_ref, *outs):
    u = (sa[...].astype(f32) + sb[...].astype(f32)) * g_ref[...].astype(f32)
    rs = rs_ref[0, 0].T
    xh = (x_ref[0, 0].astype(f32) - mu_ref[0, 0].T) * rs
    v = u - jnp.mean(u, axis=1, keepdims=True) - xh * jnp.mean(u * xh, axis=1, keepdims=True)
    dx = (dh_ref[...] + rs * v).astype(bf)
    outs[-2][...] = dx
    outs[-1][0, 0] = dx


def _lnb(kernel, ids, chunk, args, kinds, outs, out_kinds, alias=None, tile=128):
    r = args[0].shape[0]
    specs = {
        "flat": lambda k: pl.BlockSpec((tile, k), lambda i, s: (i, 0)),
        "own": lambda k: pl.BlockSpec((1, 1, tile, k), lambda i, s: (chunk, s[0], i, 0)),
        "stat": lambda k: pl.BlockSpec((1, 1, 1, tile), lambda i, s: (chunk, s[0], 0, i)),
        "gain": lambda k: pl.BlockSpec((1, k), lambda i, s: (0, 0)),
        "pair": lambda k: pl.BlockSpec((1, tile, k), lambda i, s: (s[0], i, 0)),
        "any": lambda k: pl.BlockSpec(memory_space=pl.ANY),
    }
    return pl.pallas_call(
        kernel,
        grid_spec=pltpu.PrefetchScalarGridSpec(
            num_scalar_prefetch=1,
            grid=(r // tile,),
            in_specs=[specs[k](a.shape[-1]) for k, a in zip(kinds, args)],
            out_specs=[specs[k](o.shape[-1]) for k, o in zip(out_kinds, outs)],
        ),
        out_shape=outs,
        input_output_aliases=alias or {},
        compiler_params=_params(32),
        cost_estimate=_cost(r * 2048 * 6000, r * 2048 * 16),
    )(ids, *args)


class _Chain:
    def __init__(self):
        self.last = None

    def tie(self, *args):
        if self.last is not None:
            *args, _ = lax.optimization_barrier((*args, self.last))
        return args if len(args) > 1 else args[0]

    def did(self, v):
        self.last = v
        return v


def solution(mesh):
    def body(x, mu1, rs1, g1, g2, dy, wqkv, wo, w1, w2):
        hl, hd, d = wo.shape
        t = x.shape[0]
        b = t // NB
        r = b // 2
        me = lax.axis_index("tp")
        core, chip = me % 2, me // 2
        ids = jnp.stack([core, chip]).astype(jnp.int32)

        def same(v):
            return lax.ppermute(v, "tp", SAME)

        def cross(v):
            return lax.ppermute(v, "tp", CROSS)

        split = lambda v: v.reshape(NB, 2, r, v.shape[-1])
        sds = jax.ShapeDtypeStruct
        order = _Chain()
        tie, did = order.tie, order.did
        chunks = list(reversed(range(NB)))

        wo2 = wo.reshape(hl * hd, d)
        wo_cross = cross(wo2)
        wo_same = same(wo2)
        wo_diag = same(wo_cross)

        xf = x.astype(f32)
        n1 = ((xf - mu1[:, None]) * rs1[:, None] * g1.astype(f32)).astype(bf)
        qkv = did(_dot(n1, wqkv).astype(bf))

        pair_rows = lambda v: v.reshape(2, r, v.shape[-1])
        o, lse, os = [None] * NB, [None] * NB, [None] * NB
        qkv_t = None
        for k in chunks:
            o[k], lse[k], qkv_t = _attn_fwd(tie(qkv), hd, k, b, qkv_t)
            did(o[k])
            o_cross = cross(o[k])
            o_same, o_diag = same(o[k]), same(o_cross)
            os[k] = [pair_rows(v) for v in (o[k], o_same, o_cross, o_diag)]

        dg = did(_dot_t(tie(dy), w2))

        x4, dy4 = split(x), split(dy)
        xh2, rs2, n2, others = [None] * NB, [None] * NB, [None] * NB, [None] * NB
        for k in chunks:
            xh2[k], rs2[k], n2[k] = _h1(
                ids, k, tie(x4), os[k], (wo2, wo_same, wo_cross, wo_diag), g2[None]
            )
            did(n2[k])
            others[k] = same(n2[k])

        sums = [None] * NB

        def mlp(k, prev):
            res = _mlp(ids, tie(n2[k]), others[k], w1, dg, k, prev)
            did(res[1])
            return res

        def partial(v4, k, w, cid):
            s_own = did(_partial(tie(v4), k, w, cid, 2))
            return s_own, cross(s_own)

        def grad(u, v, add=None, keep=False):
            p = _dot(u.T, tie(v))
            p = p if add is None else p + add
            return did(p if keep else p.astype(bf))

        dh, dhb = [None] * NB, [None] * NB

        def norm2(k):
            dh[k], own, dhb[k] = _lnb(
                _lnb2_kernel, ids, k, (tie(sums[k][0]), sums[k][1], xh2[k], rs2[k], dy4, g2[None]),
                ("flat", "flat", "flat", "flat", "own", "gain"),
                (pltpu.HBM((r, d), f32), sds((r, d), bf), sds((2, r, d), bf)), ("flat", "flat", "pair"),
            )
            did(own)
            return same(own)

        def attention(k, other, acc, full):
            dhb[k] = did(_place(ids, tie(dhb[k]), other)).reshape(b, d)
            do = did(_dot_t(tie(dhb[k]), wo2).astype(bf))
            res = _attn_bwd(ids, qkv, qkv_t, o[k], do, lse[k], acc, full, k, b, hd)
            did(res[0])
            return res

        def norm1(k, pair, dx):
            args = (tie(pair[0]), pair[1], x4, mu4, rs4, dh[k], g1[None]) + (() if dx is None else (dx,))
            own, dx = _lnb(
                _lnb1_kernel, ids, k, args, ("flat", "flat", "own", "stat", "stat", "flat", "gain", "any")[: len(args)],
                (sds((r, d), bf), sds((NB, 2, r, d), bf)), ("flat", "own"),
                None if dx is None else {8: 1},
            )
            did(own)
            return same(own), dx

        gd = mlp(1, ())
        sums[1] = partial(gd[1], 1, w1, 1)
        gl, da, n2_all = mlp(0, gd)
        dw2 = grad(gl, dy)
        other = norm2(1)
        sums[0] = partial(da, 0, w1, 2)

        mu4, rs4 = mu1.reshape(NB, 2, 1, r), rs1.reshape(NB, 2, 1, r)

        pair, full, acc = attention(1, other, None, None)
        pair1 = partial(pair, 0, wqkv, 3)
        other = norm2(0)
        dwo = grad(o[1], dhb[1], keep=True)
        pair, full = attention(0, other, acc, full)
        pair0 = partial(pair, 0, wqkv, 4)
        dw1 = grad(n2_all.reshape(t, d), da.reshape(t, -1))
        other1, dx = norm1(1, pair1, None)
        dwqkv = grad(n1, full)
        other0, dx = norm1(0, pair0, dx)
        dwo = grad(o[0], dhb[0], dwo).reshape(hl, hd, d)
        dx = _place4(ids, tie(dx), other1, 1)
        dx = _place4(ids, dx, other0, 0)
        return dx.reshape(t, d), dwqkv, dwo, dw1, dw2

    return jax.shard_map(
        body, mesh=mesh,
        in_specs=(P("dp", None), P("dp"), P("dp"), P(None), P(None), P("dp", None),
                  P(None, "tp"), P("tp", None, None), P(None, "tp"), P("tp", None)),
        out_specs=(P("dp", None), P("dp", "tp"), P(("dp", "tp"), None, None), P("dp", "tp"), P(("dp", "tp"), None)),
        check_vma=False)
```

```python
import functools

import jax
import jax.numpy as jnp
from jax import lax
from jax.experimental import pallas as pl
from jax.experimental.pallas import tpu as pltpu
from jax.sharding import PartitionSpec as P


EPS = 1.0 / 100000
LOG2E = 1.4426950408889634
f32 = jnp.float32
bf = jnp.bfloat16
NB = 2
BQ = 256
TILE = 256
MB = 2**20
SAME = [(0, 1), (1, 0), (2, 3), (3, 2)]
MESH = pl.DeviceIdType.MESH
CROSS = [(0, 2), (2, 0), (1, 3), (3, 1)]


def _dot(a, b):
    return jnp.dot(a, b, preferred_element_type=f32)


def _dot_t(a, b):
    return lax.dot_general(a, b, (((1,), (1,)), ((), ())), preferred_element_type=f32)


def _causal(n):
    return lax.broadcasted_iota(jnp.int32, (n, n), 0) >= lax.broadcasted_iota(jnp.int32, (n, n), 1)


def _params(mb=60):
    return pltpu.CompilerParams(vmem_limit_bytes=mb * MB)


def _cost(flops, nbytes):
    return pl.CostEstimate(flops=int(flops), bytes_accessed=int(nbytes), transcendentals=0)


def _fwd_kernel(*refs, hd, r0, r1, first):
    if first:
        qkv_ref, o_ref, lse_ref, tr_ref = refs
        for i in range(r0 // BQ):
            rows = slice(i * BQ, (i + 1) * BQ)
            tr_ref[0, :, rows] = qkv_ref[rows, :].T
    else:
        qkv_ref, tr_ref, o_ref, lse_ref = refs
    c = LOG2E * hd**-0.5
    for i in range(r0 // BQ, r1 // BQ):
        w = (i + 1) * BQ
        rows = slice(i * BQ, w)
        loc = slice(i * BQ - r0, w - r0)
        blk = qkv_ref[rows, :]
        if first:
            tr_ref[0, :, rows] = blk.T
        scores = []
        for h in range(2):
            q = blk[:, 3 * hd * h : 3 * hd * h + hd]
            kt = slice(3 * hd * h + hd, 3 * hd * h + 2 * hd)
            s = _dot(q, tr_ref[0, kt, :w])
            d = jnp.where(_causal(BQ), s[:, w - BQ :], -jnp.inf)
            scores.append(jnp.concatenate([s[:, : w - BQ], d], 1) if i else d)
        cols, ps = [], []
        for s in scores:
            m = jnp.max(s, axis=1, keepdims=True)
            p = jnp.exp2((s - m) * c)
            l = jnp.sum(p, axis=1, keepdims=True)
            cols += [m * c + jnp.log2(l), 1.0 / l]
            ps.append(p.astype(bf))
        st = jnp.concatenate(cols, 1).T
        outs = []
        for h in range(2):
            vt = slice(3 * hd * h + 2 * hd, 3 * hd * h + 3 * hd)
            outs.append((_dot_t(tr_ref[0, vt, :w], ps[h]) * st[2 * h + 1 : 2 * h + 2]).astype(bf))
            lse_ref[0, h : h + 1, loc] = st[2 * h : 2 * h + 1]
        o_ref[loc, :] = jnp.concatenate(outs, 0).T


def _attn_fwd(qkv, hd, chunk, b, tr):
    t, w = qkv.shape
    npair = w // (6 * hd)
    r0, r1 = chunk * b, (chunk + 1) * b
    first = tr is None
    trans = pl.BlockSpec((1, 6 * hd, r1), lambda p: (p, 0, 0))
    res = pl.pallas_call(
        functools.partial(_fwd_kernel, hd=hd, r0=r0, r1=r1, first=first),
        grid=(npair,),
        in_specs=[pl.BlockSpec((r1, 6 * hd), lambda p: (0, p))] + ([] if first else [trans]),
        out_specs=[pl.BlockSpec((b, 2 * hd), lambda p: (0, p)), pl.BlockSpec((1, 2, b), lambda p: (p, 0, 0))]
        + ([trans] if first else []),
        out_shape=[jax.ShapeDtypeStruct((b, npair * 2 * hd), bf), jax.ShapeDtypeStruct((npair, 2, b), f32)]
        + ([jax.ShapeDtypeStruct((npair, 6 * hd, t), bf)] if first else []),
        compiler_params=_params(32),
        cost_estimate=_cost(npair * 2 * b * (r0 + r1) * 1200, npair * 2 * t * hd * 16),
    )(qkv, *([] if first else [tr]))
    return (*res, tr)[:3]


def _bwd_kernel(*refs, hd, r0, r1, has_in, has_out):
    ids, qkv_ref, tr_ref, o_ref, do_ref, lse_ref = refs[:6]
    refs = refs[6:]
    acc_in = None
    if has_in:
        acc_in, _ = refs[:2]
        refs = refs[2:]
    pair_ref, full_ref = refs[:2]
    refs = refs[2:]
    acc_out = None
    if has_out:
        acc_out = refs[0]
        refs = refs[1:]
    (g_t,) = refs
    sc = hd**-0.5
    c = LOG2E * sc
    if has_in:
        g_t[...] = acc_in[0]
    for i in reversed(range(r0 // BQ, r1 // BQ)):
        w = (i + 1) * BQ
        rows = slice(i * BQ, w)
        loc = slice(i * BQ - r0, w - r0)
        blk = qkv_ref[loc, 0 : 4 * hd]
        do2 = do_ref[loc, :]
        do_t = do2.T
        lse = lse_ref[0, :, loc].T
        prod = do2.astype(f32) * o_ref[loc, :].astype(f32)
        sd = []
        for h in range(2):
            b = 3 * hd * h
            s = _dot(blk[:, b : b + hd], tr_ref[0, b + hd : b + 2 * hd, :w])
            dp = _dot(do2[:, h * hd : (h + 1) * hd], tr_ref[0, b + 2 * hd : b + 3 * hd, :w])
            sd.append((s, dp))
        ew = []
        for h in range(2):
            s, dp = sd[h]
            p = jnp.exp2(s * c - lse[:, h : h + 1])
            d = jnp.where(_causal(BQ), p[:, w - BQ :], 0.0)
            p = jnp.concatenate([p[:, : w - BQ], d], 1) if i else d
            delta = jnp.sum(prod[:, h * hd : (h + 1) * hd], axis=1, keepdims=True)
            ew.append((p.astype(bf), (p * (dp - delta)).astype(bf)))
        outs = []
        for h in range(2):
            p, ds = ew[h]
            b = 3 * hd * h
            dv = _dot(do_t[h * hd : (h + 1) * hd], p)
            dk = _dot(tr_ref[0, b : b + hd, rows], ds)
            dq = _dot_t(tr_ref[0, b + hd : b + 2 * hd, :w], ds)
            kr = slice(2 * hd * h, 2 * hd * h + hd)
            vr = slice(2 * hd * h + hd, 2 * hd * h + 2 * hd)
            if w == r1 and not has_in:
                g_t[kr, :] = dk
                g_t[vr, :] = dv
            else:
                g_t[kr, :w] += dk
                g_t[vr, :w] += dv
            outs += [(dq * sc).astype(bf), (g_t[kr, rows] * sc).astype(bf), g_t[vr, rows].astype(bf)]
        full_ref[loc, :] = jnp.concatenate(outs, 0).T
    half = (r1 - r0) // 2
    pair_ref[0, 0] = full_ref[pl.ds(pl.multiple_of(ids[0] * half, half), half), :]
    pair_ref[0, 1] = full_ref[pl.ds(pl.multiple_of((1 - ids[0]) * half, half), half), :]
    if has_out:
        acc_out[0] = g_t[:, :r0]


def _attn_bwd(ids, qkv, tr, o, do, lse, acc, full, chunk, b, hd):
    t, w = qkv.shape
    npair = w // (6 * hd)
    r0, r1 = chunk * b, (chunk + 1) * b
    has_in, has_out = acc is not None, r0 > 0
    in_specs = [
        pl.BlockSpec((b, 6 * hd), lambda p, s: (chunk, p)),
        pl.BlockSpec((1, 6 * hd, r1), lambda p, s: (p, 0, 0)),
        pl.BlockSpec((b, 2 * hd), lambda p, s: (0, p)),
        pl.BlockSpec((b, 2 * hd), lambda p, s: (0, p)),
        pl.BlockSpec((1, 2, b), lambda p, s: (p, 0, 0)),
    ]
    args = [qkv, tr, o, do, lse]
    alias = {}
    if has_in:
        in_specs += [pl.BlockSpec((1, 4 * hd, r1), lambda p, s: (p, 0, 0)), pl.BlockSpec(memory_space=pl.ANY)]
        args += [acc, full]
        alias = {7: 1}
    out_specs = [pl.BlockSpec((1, 2, b // 2, 6 * hd), lambda p, s: (0, 0, 0, p)), pl.BlockSpec((b, 6 * hd), lambda p, s: (chunk, p))]
    out_shape = [jax.ShapeDtypeStruct((1, 2, b // 2, w), bf), pltpu.HBM((t, w), bf)]
    if has_out:
        out_specs.append(pl.BlockSpec((1, 4 * hd, r0), lambda p, s: (p, 0, 0)))
        out_shape.append(pltpu.HBM((npair, 4 * hd, r0), f32))
    work = npair * 2 * b * (r0 + r1)
    return pl.pallas_call(
        functools.partial(_bwd_kernel, hd=hd, r0=r0, r1=r1, has_in=has_in, has_out=has_out),
        grid_spec=pltpu.PrefetchScalarGridSpec(
            num_scalar_prefetch=1,
            grid=(npair,),
            in_specs=in_specs,
            out_specs=out_specs,
            scratch_shapes=[pltpu.VMEM((4 * hd, r1), f32)],
        ),
        out_shape=out_shape,
        input_output_aliases=alias,
        compiler_params=_params(44),
        cost_estimate=_cost(work * 1500, 3 * t * w),
    )(ids, *args)


def _h1_kernel(ids, x_ref, oa, ob, oc, od, wa, wb, wc, wd, g_ref, xh_ref, rs_ref, own_ref, acc):
    def run(first, second):
        acc[...] = sum(_dot(o[0], w[...]) for o, w in first + second)

    near, far = [(oa, wa), (ob, wb)], [(oc, wc), (od, wd)]

    @pl.when(ids[1] == 0)
    def _():
        run(near, far)

    @pl.when(ids[1] != 0)
    def _():
        run(far, near)

    h1 = x_ref[0, 0].astype(f32) + acc[...]
    xc = h1 - jnp.mean(h1, axis=1, keepdims=True)
    rs = lax.rsqrt(jnp.mean(xc * xc, axis=1, keepdims=True) + EPS)
    xh = xc * rs
    n2 = (xh * g_ref[...].astype(f32)).astype(bf)
    xh_ref[...] = xh
    rs_ref[...] = jnp.broadcast_to(rs, (rs.shape[0], 128))
    own_ref[...] = n2


def _h1(ids, chunk, x4, os, ws, g2):
    _, _, r, d = x4.shape
    k = os[0].shape[-1]
    flat = lambda n: pl.BlockSpec((TILE, n), lambda i, s: (i, 0))
    const = lambda shape: pl.BlockSpec(shape, lambda i, s: (0, 0), pipeline_mode=pl.Buffered(1))
    return pl.pallas_call(
        _h1_kernel,
        grid_spec=pltpu.PrefetchScalarGridSpec(
            num_scalar_prefetch=1,
            grid=(r // TILE,),
            in_specs=[pl.BlockSpec((1, 1, TILE, d), lambda i, s: (chunk, s[0], i, 0))]
            + [pl.BlockSpec((1, TILE, k), lambda i, s: (s[0], i, 0))] * 4
            + [const((k, d))] * 4
            + [const((1, d))],
            out_specs=[flat(d), flat(128), flat(d)],
            scratch_shapes=[pltpu.VMEM((TILE, d), f32)],
        ),
        out_shape=[
            jax.ShapeDtypeStruct((r, d), f32),
            jax.ShapeDtypeStruct((r, 128), f32),
            jax.ShapeDtypeStruct((r, d), bf),
        ],
        compiler_params=_params(32),
        cost_estimate=_cost(8 * r * d * k, 20 * MB),
    )(ids, x4, *os, *ws, g2)


GC0 = 0.7978845608028654
GC1 = 0.044715


def _mlp_kernel(ids, own_n, other_n, w_ref, dg_ref, *refs):
    gl_ref, da_ref, n_ref = refs[-3:]
    sub = own_n.shape[0]
    core = ids[0]
    for half, at, src in ((0, core, own_n), (1, 1 - core, other_n)):
        rows = pl.ds(pl.multiple_of(at * sub, sub), sub)
        a = _dot(src[...], w_ref[...])
        a2 = a * a
        h = 0.5 + 0.5 * jnp.tanh(a * (GC0 + GC0 * GC1 * a2))
        gl_ref[rows, :] = (a * h).astype(bf)
        slope = h + a * (h * (1.0 - h)) * (2.0 * GC0 + 6.0 * GC0 * GC1 * a2)
        da_ref[0, half] = (dg_ref[rows, :] * slope).astype(bf)

    @pl.when(pl.program_id(0) == 0)
    def _():
        n_ref[0, 0] = own_n[...]
        n_ref[0, 1] = other_n[...]


def _mlp(ids, own, other, w1, dg, chunk, prev, bn=512):
    r, d = own.shape
    t, f = dg.shape
    spec = pl.BlockSpec((2 * r, bn), lambda j, s: (chunk, j))
    pair = lambda k, f: pl.BlockSpec((1, 2, r, k), f)
    rows = pl.BlockSpec((r, d), lambda j, s: (0, 0), pipeline_mode=pl.Buffered(1))
    return pl.pallas_call(
        _mlp_kernel,
        grid_spec=pltpu.PrefetchScalarGridSpec(
            num_scalar_prefetch=1,
            grid=(f // bn,),
            in_specs=[rows, rows, pl.BlockSpec((d, bn), lambda j, s: (0, j)), spec]
            + [pl.BlockSpec(memory_space=pl.ANY)] * len(prev),
            out_specs=[spec, pair(bn, lambda j, s: (chunk, 0, 0, j)), pair(d, lambda j, s: (chunk, 0, 0, 0))],
        ),
        out_shape=[
            pltpu.HBM((t, f), bf),
            pltpu.HBM((NB, 2, r, f), bf),
            pltpu.HBM((NB, 2, r, d), bf),
        ],
        input_output_aliases={5: 0, 6: 1, 7: 2} if prev else {},
        compiler_params=_params(48),
        cost_estimate=_cost(4 * r * d * f * 1.3, 4 * r * f * 8),
    )(ids, own, other, w1, dg, *prev)


def _partial_kernel(v_ref, w_ref, out_ref, sent, got, send_sem, recv_sem, *, nt):
    j = pl.program_id(0)
    me = lax.axis_index("tp")
    peer = {"tp": me + 1 - 2 * lax.rem(me, 2)}

    def copy(i):
        return pltpu.make_async_remote_copy(
            src_ref=sent.at[i], dst_ref=got.at[i], send_sem=send_sem.at[i], recv_sem=recv_sem.at[i],
            device_id=peer, device_id_type=MESH,
        )

    @pl.when(j == 0)
    def _():
        barrier = pltpu.get_barrier_semaphore()
        pl.semaphore_signal(barrier, inc=1, device_id=peer, device_id_type=MESH)
        pl.semaphore_wait(barrier, 1)

    @pl.when((j >= 1) & (j <= nt))
    def _():
        copy(j - 1).start()

    @pl.when(j < nt)
    def _():
        sent[j] = _dot_t(v_ref[0, 0], w_ref[...]).astype(bf)

    @pl.when(j >= nt)
    def _():
        p = _dot_t(v_ref[0, 0], w_ref[...])
        copy(j - nt).wait_recv()
        out_ref[...] = (p + got[j - nt].astype(f32)).astype(bf)

    @pl.when(j == 2 * nt - 1)
    def _():
        for i in range(nt):
            copy(i).wait_send()


def _partial(v4, chunk, w, cid, nt):
    _, _, r, k = v4.shape
    n = w.shape[0]
    bn = n // nt
    return pl.pallas_call(
        functools.partial(_partial_kernel, nt=nt),
        grid=(2 * nt,),
        in_specs=[
            pl.BlockSpec((1, 1, r, k), lambda j: (chunk, 1 - j // nt, 0, 0)),
            pl.BlockSpec((bn, k), lambda j: (lax.rem(j, nt), 0)),
        ],
        out_specs=pl.BlockSpec((r, bn), lambda j: (0, jnp.maximum(j - nt, 0))),
        out_shape=jax.ShapeDtypeStruct((r, n), bf),
        scratch_shapes=[
            pltpu.VMEM((nt, r, bn), bf),
            pltpu.VMEM((nt, r, bn), bf),
            pltpu.SemaphoreType.DMA((nt,)),
            pltpu.SemaphoreType.DMA((nt,)),
        ],
        compiler_params=pltpu.CompilerParams(vmem_limit_bytes=44 * MB, collective_id=cid, has_side_effects=True),
        cost_estimate=_cost(4 * r * k * n, 6 * r * k + 2 * n * k),
    )(v4, w)


def _place_kernel(ids, v_ref, _, buf_ref):
    buf_ref[0] = v_ref[...]


def _place(ids, buf, v):
    r, d = v.shape
    return pl.pallas_call(
        _place_kernel,
        grid_spec=pltpu.PrefetchScalarGridSpec(
            num_scalar_prefetch=1,
            grid=(r // TILE,),
            in_specs=[pl.BlockSpec((TILE, d), lambda i, s: (i, 0)), pl.BlockSpec(memory_space=pl.ANY)],
            out_specs=pl.BlockSpec((1, TILE, d), lambda i, s: (1 - s[0], i, 0)),
        ),
        out_shape=jax.ShapeDtypeStruct(buf.shape, buf.dtype),
        input_output_aliases={2: 0},
        compiler_params=_params(32),
        cost_estimate=_cost(r * d * 1000, 2 * r * d * 2),
    )(ids, v, buf)


def _place4_kernel(ids, v_ref, _, buf_ref):
    buf_ref[0, 0] = v_ref[...]


def _place4(ids, buf, v, chunk):
    r, d = v.shape
    return pl.pallas_call(
        _place4_kernel,
        grid_spec=pltpu.PrefetchScalarGridSpec(
            num_scalar_prefetch=1,
            grid=(r // TILE,),
            in_specs=[pl.BlockSpec((TILE, d), lambda i, s: (i, 0)), pl.BlockSpec(memory_space=pl.ANY)],
            out_specs=pl.BlockSpec((1, 1, TILE, d), lambda i, s: (chunk, 1 - s[0], i, 0)),
        ),
        out_shape=jax.ShapeDtypeStruct(buf.shape, buf.dtype),
        input_output_aliases={2: 0},
        compiler_params=_params(32),
        cost_estimate=_cost(r * d * 1000, 2 * r * d * 2),
    )(ids, v, buf)


def _lnb2_kernel(ids, sa, sb, xh_ref, rs_ref, dy_ref, g_ref, dh_ref, own_ref, full_ref):
    u = (sa[...].astype(f32) + sb[...].astype(f32)) * g_ref[...].astype(f32)
    xh = xh_ref[...]
    v = u - jnp.mean(u, axis=1, keepdims=True) - xh * jnp.mean(u * xh, axis=1, keepdims=True)
    dh = dy_ref[0, 0].astype(f32) + rs_ref[:, :1] * v
    dhb = dh.astype(bf)
    dh_ref[...] = dh
    own_ref[...] = dhb
    full_ref[0] = dhb


def _lnb1_kernel(ids, sa, sb, x_ref, mu_ref, rs_ref, dh_ref, g_ref, *outs):
    u = (sa[...].astype(f32) + sb[...].astype(f32)) * g_ref[...].astype(f32)
    rs = rs_ref[0, 0].T
    xh = (x_ref[0, 0].astype(f32) - mu_ref[0, 0].T) * rs
    v = u - jnp.mean(u, axis=1, keepdims=True) - xh * jnp.mean(u * xh, axis=1, keepdims=True)
    dx = (dh_ref[...] + rs * v).astype(bf)
    outs[-2][...] = dx
    outs[-1][0, 0] = dx


def _lnb(kernel, ids, chunk, args, kinds, outs, out_kinds, alias=None, tile=256):
    r = args[0].shape[0]
    specs = {
        "flat": lambda k: pl.BlockSpec((tile, k), lambda i, s: (i, 0)),
        "own": lambda k: pl.BlockSpec((1, 1, tile, k), lambda i, s: (chunk, s[0], i, 0)),
        "stat": lambda k: pl.BlockSpec((1, 1, 1, tile), lambda i, s: (chunk, s[0], 0, i)),
        "gain": lambda k: pl.BlockSpec((1, k), lambda i, s: (0, 0)),
        "pair": lambda k: pl.BlockSpec((1, tile, k), lambda i, s: (s[0], i, 0)),
        "any": lambda k: pl.BlockSpec(memory_space=pl.ANY),
    }
    return pl.pallas_call(
        kernel,
        grid_spec=pltpu.PrefetchScalarGridSpec(
            num_scalar_prefetch=1,
            grid=(r // tile,),
            in_specs=[specs[k](a.shape[-1]) for k, a in zip(kinds, args)],
            out_specs=[specs[k](o.shape[-1]) for k, o in zip(out_kinds, outs)],
        ),
        out_shape=outs,
        input_output_aliases=alias or {},
        compiler_params=_params(32),
        cost_estimate=_cost(r * 2048 * 6000, r * 2048 * 16),
    )(ids, *args)


class _Chain:
    def __init__(self):
        self.last = None

    def tie(self, *args):
        if self.last is not None:
            *args, _ = lax.optimization_barrier((*args, self.last))
        return args if len(args) > 1 else args[0]

    def did(self, v):
        self.last = v
        return v


def solution(mesh):
    def body(x, mu1, rs1, g1, g2, dy, wqkv, wo, w1, w2):
        hl, hd, d = wo.shape
        t = x.shape[0]
        b = t // NB
        r = b // 2
        me = lax.axis_index("tp")
        core, chip = me % 2, me // 2
        ids = jnp.stack([core, chip]).astype(jnp.int32)

        def same(v):
            return lax.ppermute(v, "tp", SAME)

        def cross(v):
            return lax.ppermute(v, "tp", CROSS)

        split = lambda v: v.reshape(NB, 2, r, v.shape[-1])
        sds = jax.ShapeDtypeStruct
        order = _Chain()
        tie, did = order.tie, order.did
        chunks = list(reversed(range(NB)))

        wo2 = wo.reshape(hl * hd, d)
        wo_cross = cross(wo2)
        wo_same = same(wo2)
        wo_diag = same(wo_cross)

        xf = x.astype(f32)
        n1 = ((xf - mu1[:, None]) * rs1[:, None] * g1.astype(f32)).astype(bf)
        qkv = did(_dot(n1, wqkv).astype(bf))

        pair_rows = lambda v: v.reshape(2, r, v.shape[-1])
        o, lse, os = [None] * NB, [None] * NB, [None] * NB
        qkv_t = None
        for k in chunks:
            o[k], lse[k], qkv_t = _attn_fwd(tie(qkv), hd, k, b, qkv_t)
            did(o[k])
            o_cross = cross(o[k])
            o_same, o_diag = same(o[k]), same(o_cross)
            os[k] = [pair_rows(v) for v in (o[k], o_same, o_cross, o_diag)]

        dg = did(_dot_t(tie(dy), w2))

        x4, dy4 = split(x), split(dy)
        xh2, rs2, n2, others = [None] * NB, [None] * NB, [None] * NB, [None] * NB
        for k in chunks:
            xh2[k], rs2[k], n2[k] = _h1(
                ids, k, tie(x4), os[k], (wo2, wo_same, wo_cross, wo_diag), g2[None]
            )
            did(n2[k])
            others[k] = same(n2[k])

        sums = [None] * NB

        def mlp(k, prev):
            res = _mlp(ids, tie(n2[k]), others[k], w1, dg, k, prev)
            did(res[1])
            return res

        def partial(v4, k, w, cid):
            s_own = did(_partial(tie(v4), k, w, cid, 2))
            return s_own, cross(s_own)

        def grad(u, v, add=None, keep=False):
            p = _dot(u.T, tie(v))
            p = p if add is None else p + add
            return did(p if keep else p.astype(bf))

        dh, dhb = [None] * NB, [None] * NB

        def norm2(k):
            dh[k], own, dhb[k] = _lnb(
                _lnb2_kernel, ids, k, (tie(sums[k][0]), sums[k][1], xh2[k], rs2[k], dy4, g2[None]),
                ("flat", "flat", "flat", "flat", "own", "gain"),
                (pltpu.HBM((r, d), f32), sds((r, d), bf), sds((2, r, d), bf)), ("flat", "flat", "pair"),
            )
            did(own)
            return same(own)

        def attention(k, other, acc, full):
            dhb[k] = did(_place(ids, tie(dhb[k]), other)).reshape(b, d)
            do = did(_dot_t(tie(dhb[k]), wo2).astype(bf))
            res = _attn_bwd(ids, qkv, qkv_t, o[k], do, lse[k], acc, full, k, b, hd)
            did(res[0])
            return res

        def norm1(k, pair, dx):
            args = (tie(pair[0]), pair[1], x4, mu4, rs4, dh[k], g1[None]) + (() if dx is None else (dx,))
            own, dx = _lnb(
                _lnb1_kernel, ids, k, args, ("flat", "flat", "own", "stat", "stat", "flat", "gain", "any")[: len(args)],
                (sds((r, d), bf), sds((NB, 2, r, d), bf)), ("flat", "own"),
                None if dx is None else {8: 1},
            )
            did(own)
            return same(own), dx

        gd = mlp(1, ())
        sums[1] = partial(gd[1], 1, w1, 1)
        gl, da, n2_all = mlp(0, gd)
        dw2 = grad(gl, dy)
        other = norm2(1)
        sums[0] = partial(da, 0, w1, 2)

        mu4, rs4 = mu1.reshape(NB, 2, 1, r), rs1.reshape(NB, 2, 1, r)

        pair, full, acc = attention(1, other, None, None)
        pair1 = partial(pair, 0, wqkv, 3)
        other = norm2(0)
        dwo = grad(o[1], dhb[1], keep=True)
        pair, full = attention(0, other, acc, full)
        pair0 = partial(pair, 0, wqkv, 4)
        dw1 = grad(n2_all.reshape(t, d), da.reshape(t, -1))
        other1, dx = norm1(1, pair1, None)
        dwqkv = grad(n1, full)
        other0, dx = norm1(0, pair0, dx)
        dwo = grad(o[0], dhb[0], dwo).reshape(hl, hd, d)
        dx = _place4(ids, tie(dx), other1, 1)
        dx = _place4(ids, dx, other0, 0)
        return dx.reshape(t, d), dwqkv, dwo, dw1, dw2

    return jax.shard_map(
        body, mesh=mesh,
        in_specs=(P("dp", None), P("dp"), P("dp"), P(None), P(None), P("dp", None),
                  P(None, "tp"), P("tp", None, None), P(None, "tp"), P("tp", None)),
        out_specs=(P("dp", None), P("dp", "tp"), P(("dp", "tp"), None, None), P("dp", "tp"), P(("dp", "tp"), None)),
        check_vma=False)
```
